32 devices in a mesh: gx: 2 (over x), gy: 4 (over z), gz: 4 (over y, core).
Axes of the slice: x: 2, y: 2, z: 4, core: 2. Of those that a mesh axis runs over, the one named last changes fastest.
Arguments:
- populations: float32 [39, 16, 96, 512], P(None, 'gx', 'gy', 'gz'), may hold values from 0.5 to 1.5
- relax: float32 [16, 96, 512], P('gx', 'gy', 'gz'), may hold values from 0.6 to 1.9
Outputs:
- advanced: float32 [39, 16, 96, 512], P(None, 'gx', 'gy', 'gz')
The draws below stay inside these ranges and needn't reach their ends.
All inputs are finite; a program needn't handle non-finite values.
Results may differ from the reference program's by a relative error of at most 0.0001.
Values sent between devices are 32-bit elements; how exact they have to be, the bound alone decides.
A program may use at most 128 MiB of HBM per device.

```python
import math
import jax
import jax.numpy as jnp

Q = 39
STEPS = 1
NX = 16
NY = 96
NZ = 512


def steps_of(stream_key, shape, cuts, least, high):
    level, own = 1.0, jax.random.fold_in(stream_key, 6)
    for position, blocks in cuts:
        heights = jnp.exp(jax.random.uniform(jax.random.fold_in(own, position), (blocks,), jnp.float32, least / len(cuts), high / len(cuts)))
        level = level * jnp.repeat(heights, shape[position] // blocks).reshape([-1 if axis == position else 1 for axis in range(len(shape))])
    return level


def setup_inputs(seed: int = 0) -> dict:
    splits = jax.random.split(jax.random.key(seed), 3)
    return {
        "populations": jnp.clip(0.5 + 1.0 * jax.random.uniform(splits[0], (Q, NX, NY, NZ), jnp.float32) ** steps_of(splits[0], (Q, NX, NY, NZ), ((1, 2), (2, 4), (3, 4)), -0.2, 0.2), 0.5, 1.5),
        "relax": jnp.clip(jnp.exp(math.log(1.9) - 1.1526795 * jax.random.uniform(splits[1], (NX, NY, NZ), jnp.float32) ** steps_of(splits[1], (NX, NY, NZ), ((0, 2), (1, 4), (2, 4)), -0.2, 0.2)), 0.6, 1.9),
    }


def lattice():
    speeds = [(0, 0, 0)]
    weights = [1.0 / 12.0]
    for axis in range(3):
        for sign in (1, -1):
            vector = [0, 0, 0]
            vector[axis] = sign
            speeds.append(tuple(vector))
            weights.append(1.0 / 12.0)
    for first in (1, -1):
        for second in (1, -1):
            for third in (1, -1):
                speeds.append((first, second, third))
                weights.append(1.0 / 27.0)
    for axis in range(3):
        for sign in (2, -2):
            vector = [0, 0, 0]
            vector[axis] = sign
            speeds.append(tuple(vector))
            weights.append(2.0 / 135.0)
    for couple in ((0, 1), (0, 2), (1, 2)):
        for first in (2, -2):
            for second in (2, -2):
                vector = [0, 0, 0]
                vector[couple[0]] = first
                vector[couple[1]] = second
                speeds.append(tuple(vector))
                weights.append(1.0 / 432.0)
    for axis in range(3):
        for sign in (3, -3):
            vector = [0, 0, 0]
            vector[axis] = sign
            speeds.append(tuple(vector))
            weights.append(1.0 / 1620.0)
    return speeds, weights


def collide(popul, rate):
    speeds, weights = lattice()
    acoustic_wave_rate = 2.0 / 3.0
    inverse = 1.0 / (acoustic_wave_rate ** 0.5)
    zeroth_moment_rho = sum(weights[member] * popul[member] for member in range(39))
    flux = [sum(weights[member] * speeds[member][axis] * popul[member] for member in range(39) if speeds[member][axis] != 0) for axis in range(3)]
    thermal_heat_content = sum(weights[member] * float(sum(value * value for value in speeds[member])) * popul[member] for member in range(1, 39))
    velocity = [part / zeroth_moment_rho for part in flux]
    flow_norm_square = velocity[0] * velocity[0] + velocity[1] * velocity[1] + velocity[2] * velocity[2]
    site_kinetic_heat = (thermal_heat_content / zeroth_moment_rho - flow_norm_square) / (3.0 * acoustic_wave_rate)
    scaled = [part * inverse for part in velocity]
    scaled_square = flow_norm_square / acoustic_wave_rate
    excess_quantity = site_kinetic_heat - 1.0
    results = []
    for member in range(39):
        vector = speeds[member]
        aligned = sum(vector[axis] * inverse * scaled[axis] for axis in range(3) if vector[axis] != 0) if member > 0 else jnp.zeros_like(zeroth_moment_rho)
        speed_square = float(sum(value * value for value in vector)) / acoustic_wave_rate
        aligned_square = aligned * aligned
        hermite = (1.0 + aligned
                   + 0.5 * (aligned_square - scaled_square + excess_quantity * (speed_square - 3.0))
                   + aligned * (aligned_square - 3.0 * scaled_square + 3.0 * excess_quantity * (speed_square - 5.0)) / 6.0
                   + (aligned_square * aligned_square - 6.0 * aligned_square * scaled_square + 3.0 * scaled_square * scaled_square
                      + 6.0 * excess_quantity * (aligned_square * (speed_square - 7.0) + scaled_square * (5.0 - speed_square))
                      + 3.0 * excess_quantity * excess_quantity * (speed_square * speed_square - 10.0 * speed_square + 15.0)) / 24.0)
        maxwellian_target = zeroth_moment_rho * hermite
        results.append(popul[member] - rate * (popul[member] - maxwellian_target))
    return jnp.stack(results)


def reference(populations, relax):
    speeds, weights = lattice()
    state = populations
    for number in range(STEPS):
        post = collide(state, relax)
        state = jnp.stack([jnp.roll(post[member], speeds[member], axis=(0, 1, 2)) for member in range(39)])
    return state
```

```python
import math

import jax
import jax.numpy as jnp
from jax import lax
from jax.experimental import pallas as pl
from jax.experimental.pallas import tpu as pltpu
from jax.sharding import PartitionSpec as P

MESH = pl.DeviceIdType.MESH
AXES = ("gx", "gy", "gz")
PX = 3
PY = 8
TILE = 8


def lattice():
    speeds = [(0, 0, 0)]
    weights = [1.0 / 12.0]
    for axis in range(3):
        for sign in (1, -1):
            vector = [0, 0, 0]
            vector[axis] = sign
            speeds.append(tuple(vector))
            weights.append(1.0 / 12.0)
    for first in (1, -1):
        for second in (1, -1):
            for third in (1, -1):
                speeds.append((first, second, third))
                weights.append(1.0 / 27.0)
    for axis in range(3):
        for sign in (2, -2):
            vector = [0, 0, 0]
            vector[axis] = sign
            speeds.append(tuple(vector))
            weights.append(2.0 / 135.0)
    for couple in ((0, 1), (0, 2), (1, 2)):
        for first in (2, -2):
            for second in (2, -2):
                vector = [0, 0, 0]
                vector[couple[0]] = first
                vector[couple[1]] = second
                speeds.append(tuple(vector))
                weights.append(1.0 / 432.0)
    for axis in range(3):
        for sign in (3, -3):
            vector = [0, 0, 0]
            vector[axis] = sign
            speeds.append(tuple(vector))
            weights.append(1.0 / 1620.0)
    return (speeds, weights)


SPEEDS, WEIGHTS = lattice()
Q = len(SPEEDS)
SQUARES = [sum(v * v for v in c) for c in SPEEDS]
PAIRS = [
    (m, SPEEDS.index(tuple(-v for v in SPEEDS[m])))
    for m in range(1, Q)
    if m < SPEEDS.index(tuple(-v for v in SPEEDS[m]))
]


EDGE = [
    (m, o) for m, o in PAIRS if SPEEDS[m][2] == 0 and SPEEDS[m][0] != 0
]
REST = [pair for pair in PAIRS if pair not in EDGE]


def crossing(m, x, nx):
    at = x + SPEEDS[m][0]
    return 0 if at >= nx else 1 if at < 0 else None


def slots(axis, sign, layers, keep):
    rows, start = [], 0
    for x in layers:
        for m, c in enumerate(SPEEDS):
            count = c[axis] * sign
            if count > 0 and keep(m, x):
                rows.append((m, x, start, count))
                start += count
    return rows, start


def plan(nx):
    order = []
    for x in range((nx + 1) // 2):
        order += [x] if x == nx - 1 - x else [x, nx - 1 - x]
    chunks = [order[:2], order[2:4], order[4:]]
    zcols = [
        [slots(2, sign, layers, lambda m, x: True)[0] for sign in (1, -1)]
        for layers in chunks
    ]
    kinds = [
        lambda m, x: crossing(m, x, nx) is not None and SPEEDS[m][2] == 0,
        lambda m, x: crossing(m, x, nx) is not None and SPEEDS[m][2] != 0,
        lambda m, x: crossing(m, x, nx) is None and SPEEDS[m][2] == 0,
        lambda m, x: crossing(m, x, nx) is None and SPEEDS[m][2] != 0,
    ]
    yrows, start = [], 0
    for keep in kinds:
        both = [slots(1, sign, order, keep) for sign in (1, -1)]
        size = -(-max(n for _, n in both) // TILE) * TILE
        yrows.append(([rows for rows, _ in both], start, size))
        start += size
    return order, chunks, zcols, yrows, start


def add_all(terms):
    total = terms[0]
    for term in terms[1:]:
        total = total + term
    return total


def collide(load, rate):
    sums = {k: [] for k in (1, 3, 4, 8, 9)}
    flows = {k: [[], [], []] for k in (1, 3, 4, 8, 9)}
    for m, o in PAIRS:
        up, down = load(m), load(o)
        k = SQUARES[m]
        sums[k].append(up + down)
        diff = up - down
        for axis in range(3):
            if SPEEDS[m][axis] > 0:
                flows[k][axis].append((1, diff))
            elif SPEEDS[m][axis] < 0:
                flows[k][axis].append((-1, diff))
    weight = {SQUARES[m]: WEIGHTS[m] for m in range(Q)}
    size = {1: 1, 3: 1, 4: 2, 8: 2, 9: 3}
    rest = load(0)
    groups = {k: add_all(sums[k]) for k in sums}
    rho = weight[0] * rest
    energy = None
    for k in sums:
        part = weight[k] * groups[k]
        rho = rho + part
        part = part if k == 1 else float(k) * part
        energy = part if energy is None else energy + part
    flux = []
    for axis in range(3):
        total = None
        for k in flows:
            part = None
            for sign, diff in flows[k][axis]:
                if part is None:
                    part = diff if sign > 0 else -diff
                else:
                    part = part + diff if sign > 0 else part - diff
            part = (weight[k] * size[k]) * part
            total = part if total is None else total + part
        flux.append(total)
    inverse = 1.0 / rho
    velocity = [part * inverse for part in flux]
    norm = velocity[0] * velocity[0] + velocity[1] * velocity[1] + velocity[2] * velocity[2]
    t = (energy * inverse - norm) * 0.5 - 1.0
    b = 1.5 * norm
    w = [1.5 * part for part in velocity]
    keep = 1.0 - rate
    k0 = rho * rate
    k24 = k0 * (1.0 / 24.0)
    k6 = k0 * (1.0 / 6.0)
    half_b = 0.5 * b
    kt = k0 * t
    ktb = kt * b
    ktt = kt * t
    base = k0 * (1.0 - half_b + 0.5 * half_b * half_b)
    base1 = k0 * (0.5 - 0.5 * half_b)
    baseo = k0 * (1.0 - half_b)

    def even0(s):
        return (
            base
            + kt * (0.5 * (s - 3.0))
            + ktb * (0.25 * (5.0 - s))
            + ktt * ((s * s - 10.0 * s + 15.0) / 8.0)
        )

    def emit_rest(emit):
        emit(0, keep * rest + even0(0.0))

    def emit_pairs(pairs, emit):
        for k in sums:
            chosen = [pair for pair in pairs if SQUARES[pair[0]] == k]
            if not chosen:
                continue
            s = 1.5 * k
            e0 = even0(s)
            e1 = base1 + kt * (0.25 * (s - 7.0))
            o1 = baseo + kt * (0.5 * (s - 5.0))
            for m, o in chosen:
                a = None
                for axis in range(3):
                    v = SPEEDS[m][axis]
                    if v == 0:
                        continue
                    unit = w[axis]
                    if a is None:
                        a = unit if v > 0 else -unit
                    else:
                        a = a + unit if v > 0 else a - unit
                if size[k] != 1:
                    a = float(size[k]) * a
                q = a * a
                even = e0 + q * (e1 + q * k24)
                odd = a * (o1 + q * k6)
                emit(m, keep * load(m) + (even + odd))
                emit(o, keep * load(o) + (even - odd))

    return emit_rest, emit_pairs


def kernel(
    pop, rate, ext, g, r, zs, zr, ys, yr,
    in_sem, z_ss, z_rs, y_ss, y_rs, x_ss, x_rs, ready,
):
    nx, ny, nz = pop.shape[1:]
    order, chunks, zcols, yrows, _ = plan(nx)
    groups = [(x, 1) for x in order[:4]] + [(2, nx - 4)]
    loads = [
        pltpu.make_async_copy(
            pop.at[:, pl.ds(first, count)], g.at[:, pl.ds(first, count)], in_sem.at[n]
        )
        for n, (first, count) in enumerate(groups)
    ]
    loads.append(pltpu.make_async_copy(rate, r, in_sem.at[5]))

    around = []
    for axis in AXES:
        n = lax.axis_size(axis)
        me = lax.axis_index(axis)
        around.append(({axis: lax.rem(me + 1, n)}, {axis: lax.rem(me + n - 1, n)}))
    barrier = pltpu.get_barrier_semaphore()
    greeted = (around[1][1],) + around[0] + around[2]
    for target in greeted:
        pl.semaphore_signal(barrier, inc=1, device_id=target, device_id_type=MESH)
    for n in (5, 0, 1, 2, 3, 4):
        loads[n].start()

    lane = lax.broadcasted_iota(jnp.int32, (ny, nz), 1)

    def rows_at(m):
        return pl.ds(PY + SPEEDS[m][1], ny)

    def place(m, x):
        return PX + x + SPEEDS[m][0]

    def remote(axis, d, src, dst, ss, rs):
        return pltpu.make_async_remote_copy(
            src_ref=src, dst_ref=dst, send_sem=ss, recv_sem=rs,
            device_id=around[axis][d], device_id_type=MESH,
        )

    sent = []

    def send_x(m, members, x, rows):
        d = crossing(m, x, nx)
        at = place(m, x)
        home = at - nx if d == 0 else at + nx
        start, count = rows
        which, rows = pl.ds(m, members), pl.ds(PY + start, count)
        remote(
            0, d, ext.at[which, pl.ds(at, 1), rows], ext.at[which, pl.ds(home, 1), rows],
            x_ss.at[0], x_rs.at[0],
        ).start()
        sent.append(members * count)

    def send_z(chunk):
        for d in (0, 1):
            remote(
                2, d, zs.at[chunk, d], zr.at[chunk, d], z_ss.at[0], z_rs.at[chunk]
            ).start()

    def send_y(kinds, d):
        for kind in kinds:
            _, start, size = yrows[kind]
            rows = pl.ds(start, size)
            remote(
                1, d, ys.at[d, rows], yr.at[d, rows], y_ss.at[0],
                y_rs.at[max(kind - 1, 0)],
            ).start()

    def early(m):
        v = SPEEDS[m][1]
        return (0, ny) if v == 0 else (TILE, ny - TILE) if v > 0 else (0, ny - TILE)

    def late(m):
        return (0, TILE) if SPEEDS[m][1] > 0 else (ny - TILE, TILE)

    def outgoing(x, chosen):
        return [m for m in range(Q) if crossing(m, x, nx) is not None and chosen(SPEEDS[m])]

    def send_edge(x):
        for m in outgoing(x, lambda c: c[2] == 0):
            send_x(m, 1, x, early(m))

    def send_tilted(x):
        for m in outgoing(x, lambda c: c[2] > 0):
            send_x(m, 2, x, early(m))

    def send_late(x):
        for m in outgoing(x, lambda c: c[1] != 0 and c[2] == 0):
            send_x(m, 1, x, late(m))
        for m in outgoing(x, lambda c: c[1] != 0 and c[2] > 0):
            send_x(m, 2, x, late(m))

    def work(x, chunk, packed, between):
        slot = [{m: (s, c) for m, at, s, c in zcols[chunk][d] if at == x} for d in (0, 1)]

        def emit(m, value):
            cz = SPEEDS[m][2]
            if cz:
                d = 0 if cz > 0 else 1
                start, count = slot[d][m]
                shift = (start + count if d == 0 else start) % nz
                moved = pltpu.roll(value, shift, 1) if shift else value
                mask = (lane >= start) & (lane < start + count)
                packed[d] = jnp.where(mask, moved, packed[d])
                value = pltpu.roll(value, cz % nz, 1)
            ext[m, place(m, x), rows_at(m), :] = value

        emit_rest, emit_pairs = collide(lambda m: g[m, x], r[x])
        emit_pairs(EDGE, emit)
        between()
        emit_rest(emit)
        emit_pairs(REST, emit)

    def settle_z(chunk, chosen):
        for d in (0, 1):
            base = zr[chunk, d]
            for m, x, start, count in zcols[chunk][d]:
                if not chosen(m, x):
                    continue
                shift = (start if d == 0 else start + count) % nz
                moved = pltpu.roll(base, nz - shift, 1) if shift else base
                mask = lane < count if d == 0 else lane >= nz - count
                where = (m, place(m, x), rows_at(m), slice(None))
                ext[where] = jnp.where(mask, moved, ext[where])

    def pack_y(kind):
        tables, first, _ = yrows[kind]
        for d in (0, 1):
            for m, x, start, count in tables[d]:
                edge = PY + ny if d == 0 else PY - count
                ys[d, pl.ds(first + start, count), :] = ext[
                    m, place(m, x), pl.ds(edge, count), :
                ]

    def settle_y(kind):
        tables, first, _ = yrows[kind]
        for d in (0, 1):
            for m, x, start, count in tables[d]:
                home = PY if d == 0 else PY + ny - count
                ext[m, place(m, x), pl.ds(home, count), :] = yr[
                    d, pl.ds(first + start, count), :
                ]

    def crosses(m, x):
        return crossing(m, x, nx) is not None

    def stays(m, x):
        return crossing(m, x, nx) is None

    def greet():
        pl.semaphore_wait(barrier, len(greeted))
        pl.semaphore_signal(ready, inc=1, device_id=around[1][0], device_id_type=MESH)

    loads[5].wait()
    blank = jnp.zeros((ny, nz), jnp.float32)
    for chunk, layers in enumerate(chunks):
        packed = [blank, blank]
        for n, x in enumerate(layers):
            if chunk < 2:
                loads[2 * chunk + n].wait()
            elif n == 0:
                loads[4].wait()

            def between(x=x):
                if x == order[0]:
                    greet()
                send_edge(x)

            work(x, chunk, packed, between)
        for d in (0, 1):
            zs[chunk, d] = packed[d]
        send_z(chunk)
        if chunk == 1:
            pack_y(0)
            send_y((0,), 0)
    pack_y(2)
    send_y((2,), 0)

    def wait_z(chunk):
        remote(2, 0, zs.at[chunk], zr.at[chunk], z_ss.at[0], z_rs.at[chunk]).wait_recv()

    wait_z(0)
    settle_z(0, crosses)
    for x in chunks[0]:
        send_tilted(x)
    pack_y(1)
    send_y((1,), 0)
    wait_z(1)
    settle_z(1, crosses)
    for x in chunks[1]:
        send_tilted(x)
    pl.semaphore_wait(ready, 1)
    send_y((1, 0, 2), 1)
    settle_z(0, stays)
    settle_z(1, stays)
    wait_z(2)
    settle_z(2, stays)
    pack_y(3)
    for d in (0, 1):
        send_y((3,), d)

    def wait_y(kinds):
        first = yrows[kinds[0]][1]
        size = sum(yrows[kind][2] for kind in kinds)
        part = (slice(None), pl.ds(first, size))
        remote(
            1, 0, ys.at[part], yr.at[part], y_ss.at[0], y_rs.at[max(kinds[0] - 1, 0)]
        ).wait_recv()

    wait_y((0, 1))
    settle_y(0)
    settle_y(1)
    for x in order:
        send_late(x)
    wait_y((2,))
    settle_y(2)
    wait_y((3,))
    settle_y(3)
    units = sum(sent) // ny
    layers = max(n for n in range(1, nx + 1) if units % n == 0)
    span = ext.at[pl.ds(0, units // layers), pl.ds(0, layers), pl.ds(PY, ny)]
    everything = remote(0, 0, span, span, x_ss.at[0], x_rs.at[0])
    everything.wait_recv()
    everything.wait_send()
    remote(1, 0, ys, ys, y_ss.at[0], y_rs.at[0]).wait_send()
    remote(2, 0, zs, zs, z_ss.at[0], z_rs.at[0]).wait_send()


def crop(ext, out, sem):
    nx, ny = out.shape[1:3]
    parts = 3
    share = Q // parts
    copies = [
        pltpu.make_async_copy(
            ext.at[pl.ds(n * share, share), pl.ds(PX, nx), pl.ds(PY, ny)],
            out.at[pl.ds(n * share, share)],
            sem.at[n],
        )
        for n in range(parts)
    ]
    for copy in copies:
        copy.start()
    for copy in copies:
        copy.wait()


def per_device(populations, relax):
    nx, ny, nz = relax.shape
    shape = (Q, nx + 2 * PX, ny + 2 * PY, nz)
    height = plan(nx)[4]
    f32 = jnp.float32
    dma = pltpu.SemaphoreType.DMA
    any_space = pl.BlockSpec(memory_space=pl.ANY)
    room = 67043328 - 4 * math.prod(shape) - 32768
    ext = pl.pallas_call(
        kernel,
        out_shape=pltpu.VMEM(shape, f32),
        in_specs=[pl.BlockSpec(memory_space=pltpu.HBM)] * 2,
        out_specs=pl.BlockSpec(memory_space=pltpu.VMEM),
        scratch_shapes=[
            pltpu.VMEM((Q, nx, ny, nz), f32),
            pltpu.VMEM((nx, ny, nz), f32),
            pltpu.VMEM((3, 2, ny, nz), f32),
            pltpu.VMEM((3, 2, ny, nz), f32),
            pltpu.VMEM((2, height, nz), f32),
            pltpu.VMEM((2, height, nz), f32),
            dma((6,)),
            dma((1,)), dma((3,)),
            dma((1,)), dma((3,)),
            dma((1,)), dma((1,)),
            pltpu.SemaphoreType.REGULAR,
        ],
        compiler_params=pltpu.CompilerParams(
            collective_id=0, has_side_effects=True, vmem_limit_bytes=room
        ),
    )(populations, relax)
    return pl.pallas_call(
        crop,
        out_shape=jax.ShapeDtypeStruct((Q, nx, ny, nz), f32),
        in_specs=[any_space],
        out_specs=any_space,
        scratch_shapes=[dma((3,))],
        compiler_params=pltpu.CompilerParams(vmem_limit_bytes=2**20),
    )(ext)


def solution(mesh):
    return jax.shard_map(
        per_device,
        mesh=mesh,
        in_specs=(P(None, "gx", "gy", "gz"), P("gx", "gy", "gz")),
        out_specs=P(None, "gx", "gy", "gz"),
        check_vma=False,
    )
```

```python
import math

import jax
import jax.numpy as jnp
from jax import lax
from jax.experimental import pallas as pl
from jax.experimental.pallas import tpu as pltpu
from jax.sharding import PartitionSpec as P

MESH = pl.DeviceIdType.MESH
AXES = ("gx", "gy", "gz")
PX = 3
PY = 8
TILE = 8


def lattice():
    speeds = [(0, 0, 0)]
    weights = [1.0 / 12.0]
    for axis in range(3):
        for sign in (1, -1):
            vector = [0, 0, 0]
            vector[axis] = sign
            speeds.append(tuple(vector))
            weights.append(1.0 / 12.0)
    for first in (1, -1):
        for second in (1, -1):
            for third in (1, -1):
                speeds.append((first, second, third))
                weights.append(1.0 / 27.0)
    for axis in range(3):
        for sign in (2, -2):
            vector = [0, 0, 0]
            vector[axis] = sign
            speeds.append(tuple(vector))
            weights.append(2.0 / 135.0)
    for couple in ((0, 1), (0, 2), (1, 2)):
        for first in (2, -2):
            for second in (2, -2):
                vector = [0, 0, 0]
                vector[couple[0]] = first
                vector[couple[1]] = second
                speeds.append(tuple(vector))
                weights.append(1.0 / 432.0)
    for axis in range(3):
        for sign in (3, -3):
            vector = [0, 0, 0]
            vector[axis] = sign
            speeds.append(tuple(vector))
            weights.append(1.0 / 1620.0)
    return (speeds, weights)


SPEEDS, WEIGHTS = lattice()
Q = len(SPEEDS)
SQUARES = [sum(v * v for v in c) for c in SPEEDS]
PAIRS = [
    (m, SPEEDS.index(tuple(-v for v in SPEEDS[m])))
    for m in range(1, Q)
    if m < SPEEDS.index(tuple(-v for v in SPEEDS[m]))
]


EDGE = [
    (m, o) for m, o in PAIRS if SPEEDS[m][2] == 0 and SPEEDS[m][0] != 0
]
REST = [pair for pair in PAIRS if pair not in EDGE]


def crossing(m, x, nx):
    at = x + SPEEDS[m][0]
    return 0 if at >= nx else 1 if at < 0 else None


def slots(axis, sign, layers, keep):
    rows, start = [], 0
    for x in layers:
        for m, c in enumerate(SPEEDS):
            count = c[axis] * sign
            if count > 0 and keep(m, x):
                rows.append((m, x, start, count))
                start += count
    return rows, start


def plan(nx):
    order = []
    for x in range((nx + 1) // 2):
        order += [x] if x == nx - 1 - x else [x, nx - 1 - x]
    chunks = [order[:2], order[2:4], order[4:]]
    zcols = [
        [slots(2, sign, layers, lambda m, x: True)[0] for sign in (1, -1)]
        for layers in chunks
    ]
    near = set(order[:4])
    kinds = [
        lambda m, x: crossing(m, x, nx) is not None,
        lambda m, x: crossing(m, x, nx) is None and x in near,
        lambda m, x: crossing(m, x, nx) is None and x not in near,
    ]
    yrows, start = [], 0
    for keep in kinds:
        both = [slots(1, sign, order, keep) for sign in (1, -1)]
        size = -(-max(n for _, n in both) // TILE) * TILE
        yrows.append(([rows for rows, _ in both], start, size))
        start += size
    return order, chunks, zcols, yrows, start


def add_all(terms):
    total = terms[0]
    for term in terms[1:]:
        total = total + term
    return total


def collide(load, rate):
    sums = {k: [] for k in (1, 3, 4, 8, 9)}
    flows = {k: [[], [], []] for k in (1, 3, 4, 8, 9)}
    for m, o in PAIRS:
        up, down = load(m), load(o)
        k = SQUARES[m]
        sums[k].append(up + down)
        diff = up - down
        for axis in range(3):
            if SPEEDS[m][axis] > 0:
                flows[k][axis].append((1, diff))
            elif SPEEDS[m][axis] < 0:
                flows[k][axis].append((-1, diff))
    weight = {SQUARES[m]: WEIGHTS[m] for m in range(Q)}
    size = {1: 1, 3: 1, 4: 2, 8: 2, 9: 3}
    rest = load(0)
    groups = {k: add_all(sums[k]) for k in sums}
    rho = weight[0] * rest
    energy = None
    for k in sums:
        part = weight[k] * groups[k]
        rho = rho + part
        part = part if k == 1 else float(k) * part
        energy = part if energy is None else energy + part
    flux = []
    for axis in range(3):
        total = None
        for k in flows:
            part = None
            for sign, diff in flows[k][axis]:
                if part is None:
                    part = diff if sign > 0 else -diff
                else:
                    part = part + diff if sign > 0 else part - diff
            part = (weight[k] * size[k]) * part
            total = part if total is None else total + part
        flux.append(total)
    inverse = 1.0 / rho
    velocity = [part * inverse for part in flux]
    norm = velocity[0] * velocity[0] + velocity[1] * velocity[1] + velocity[2] * velocity[2]
    t = (energy * inverse - norm) * 0.5 - 1.0
    b = 1.5 * norm
    w = [1.5 * part for part in velocity]
    keep = 1.0 - rate
    k0 = rho * rate
    k24 = k0 * (1.0 / 24.0)
    k6 = k0 * (1.0 / 6.0)
    half_b = 0.5 * b
    kt = k0 * t
    ktb = kt * b
    ktt = kt * t
    base = k0 * (1.0 - half_b + 0.5 * half_b * half_b)
    base1 = k0 * (0.5 - 0.5 * half_b)
    baseo = k0 * (1.0 - half_b)

    def even0(s):
        return (
            base
            + kt * (0.5 * (s - 3.0))
            + ktb * (0.25 * (5.0 - s))
            + ktt * ((s * s - 10.0 * s + 15.0) / 8.0)
        )

    def emit_rest(emit):
        emit(0, keep * rest + even0(0.0))

    def emit_pairs(pairs, emit):
        for k in sums:
            chosen = [pair for pair in pairs if SQUARES[pair[0]] == k]
            if not chosen:
                continue
            s = 1.5 * k
            e0 = even0(s)
            e1 = base1 + kt * (0.25 * (s - 7.0))
            o1 = baseo + kt * (0.5 * (s - 5.0))
            for m, o in chosen:
                a = None
                for axis in range(3):
                    v = SPEEDS[m][axis]
                    if v == 0:
                        continue
                    unit = w[axis]
                    if a is None:
                        a = unit if v > 0 else -unit
                    else:
                        a = a + unit if v > 0 else a - unit
                if size[k] != 1:
                    a = float(size[k]) * a
                q = a * a
                even = e0 + q * (e1 + q * k24)
                odd = a * (o1 + q * k6)
                emit(m, keep * load(m) + (even + odd))
                emit(o, keep * load(o) + (even - odd))

    return emit_rest, emit_pairs


def kernel(
    pop, rate, ext, g, r, zs, zr, zd, ys, yr,
    in_sem, z_ss, z_rs, d_ss, d_rs, y_ss, y_rs, x_ss, x_rs, ready,
):
    nx, ny, nz = pop.shape[1:]
    order, chunks, zcols, yrows, _ = plan(nx)
    groups = [(x, 1) for x in order[:4]] + [(2, nx - 4)]
    loads = [
        pltpu.make_async_copy(
            pop.at[:, pl.ds(first, count)], g.at[:, pl.ds(first, count)], in_sem.at[n]
        )
        for n, (first, count) in enumerate(groups)
    ]
    loads.append(pltpu.make_async_copy(rate, r, in_sem.at[5]))

    around, above = [], []
    for axis in AXES:
        n = lax.axis_size(axis)
        me = lax.axis_index(axis)
        near = (lax.rem(me + 1, n), lax.rem(me + n - 1, n))
        around.append(tuple({axis: at} for at in near))
        above.append(tuple(jnp.where(at > me, 1, 0) for at in near))
    barrier = pltpu.get_barrier_semaphore()

    links = [
        (((0, d),), 0) for d in (0, 1)
    ] + [
        (((2, d),), 1) for d in (0, 1)
    ] + [
        (((1, d), (2, z))[: 1 if z is None else 2], 3 - d)
        for d in (0, 1) for z in (None, 0, 1)
    ]

    def at(steps):
        return {name: v for axis, d in steps for name, v in around[axis][d].items()}

    def is_above(steps):
        return above[steps[0][0]][steps[0][1]]

    def signal(semaphore, steps):
        pl.semaphore_signal(semaphore, inc=1, device_id=at(steps), device_id_type=MESH)

    def wait(semaphore, amount):
        pl.when(amount > 0)(lambda: pl.semaphore_wait(semaphore, amount))

    for steps, _ in links:
        pl.when(is_above(steps) == 1)(lambda p=steps: signal(barrier, p))
    for n in (0, 5, 1, 2, 3, 4):
        loads[n].start()
    wait(barrier, sum(1 - is_above(steps) for steps, _ in links))
    for steps, flag in links:
        pl.when(is_above(steps) == 0)(lambda p=steps, f=flag: signal(ready.at[f], p))

    def await_ready(axis, d=None):
        if axis == 1:
            wait(ready.at[2 + d], 3 * above[1][d])
        else:
            wait(ready.at[axis // 2], sum(above[axis]))

    lane = lax.broadcasted_iota(jnp.int32, (ny, nz), 1)

    def rows_at(m):
        return pl.ds(PY + SPEEDS[m][1], ny)

    def place(m, x):
        return PX + x + SPEEDS[m][0]

    def remote(steps, src, dst, ss, rs):
        return pltpu.make_async_remote_copy(
            src_ref=src, dst_ref=dst, send_sem=ss, recv_sem=rs,
            device_id=at(steps), device_id_type=MESH,
        )

    sent = []

    def send_x(m, members, x, rows):
        d = crossing(m, x, nx)
        at = place(m, x)
        home = at - nx if d == 0 else at + nx
        start, count = rows
        which, rows = pl.ds(m, members), pl.ds(PY + start, count)
        remote(
            ((0, d),), ext.at[which, pl.ds(at, 1), rows], ext.at[which, pl.ds(home, 1), rows],
            x_ss.at[0], x_rs.at[0],
        ).start()
        sent.append(members * count)

    def send_z(chunk):
        for d in (0, 1):
            remote(
                ((2, d),), zs.at[chunk, d], zr.at[chunk, d], z_ss.at[0], z_rs.at[chunk]
            ).start()

    def send_corners(first, count, d):
        part = pl.ds(first, count)
        rows = pl.ds(ny - TILE if d == 0 else 0, TILE)
        for z in (0, 1):
            remote(
                ((1, d), (2, z)), zs.at[part, z, rows], zd.at[d, part, z],
                d_ss.at[0], d_rs.at[min(first, 1)],
            ).start()

    def send_y(kind, d):
        _, start, size = yrows[kind]
        rows = pl.ds(start, size)
        remote(
            ((1, d),), ys.at[d, rows], yr.at[d, rows], y_ss.at[0], y_rs.at[kind]
        ).start()

    def early(m):
        v = SPEEDS[m][1]
        return (0, ny) if v == 0 else (TILE, ny - TILE) if v > 0 else (0, ny - TILE)

    def late(m):
        return (0, TILE) if SPEEDS[m][1] > 0 else (ny - TILE, TILE)

    def outgoing(x, chosen):
        return [m for m in range(Q) if crossing(m, x, nx) is not None and chosen(SPEEDS[m])]

    def send_edge(x):
        for m in outgoing(x, lambda c: c[2] == 0):
            send_x(m, 1, x, early(m))

    def send_tilted(x):
        for m in outgoing(x, lambda c: c[2] > 0):
            send_x(m, 2, x, early(m))

    def send_late(x, tilted):
        for m in outgoing(x, lambda c: c[1] != 0 and (c[2] > 0 if tilted else c[2] == 0)):
            send_x(m, 1 + tilted, x, late(m))

    def work(x, chunk, packed, between):
        slot = [{m: (s, c) for m, at, s, c in zcols[chunk][d] if at == x} for d in (0, 1)]

        def emit(m, value):
            cz = SPEEDS[m][2]
            if cz:
                d = 0 if cz > 0 else 1
                start, count = slot[d][m]
                shift = (start + count if d == 0 else start) % nz
                moved = pltpu.roll(value, shift, 1) if shift else value
                mask = (lane >= start) & (lane < start + count)
                packed[d] = jnp.where(mask, moved, packed[d])
                value = pltpu.roll(value, cz % nz, 1)
            ext[m, place(m, x), rows_at(m), :] = value

        emit_rest, emit_pairs = collide(lambda m: g[m, x], r[x])
        emit_pairs(EDGE, emit)
        between()
        emit_rest(emit)
        emit_pairs(REST, emit)

    def settle_z(chunk, chosen):
        for d in (0, 1):
            base = zr[chunk, d]
            for m, x, start, count in zcols[chunk][d]:
                if not chosen(m, x):
                    continue
                shift = (start if d == 0 else start + count) % nz
                moved = pltpu.roll(base, nz - shift, 1) if shift else base
                mask = lane < count if d == 0 else lane >= nz - count
                where = (m, place(m, x), rows_at(m), slice(None))
                ext[where] = jnp.where(mask, moved, ext[where])

    def pack_y(kind):
        tables, first, _ = yrows[kind]
        for d in (0, 1):
            for m, x, start, count in tables[d]:
                edge = PY + ny if d == 0 else PY - count
                ys[d, pl.ds(first + start, count), :] = ext[
                    m, place(m, x), pl.ds(edge, count), :
                ]

    def settle_y(kind, chosen):
        tables, first, _ = yrows[kind]
        for d in (0, 1):
            for m, x, start, count in tables[d]:
                if not chosen(m, x):
                    continue
                home = PY if d == 0 else PY + ny - count
                rows = yr[d, pl.ds(first + start, count), :]
                cz = SPEEDS[m][2]
                if cz:
                    z = 0 if cz > 0 else 1
                    rows = corner(d, z, m, x, rows)
                ext[m, place(m, x), pl.ds(home, count), :] = rows

    def corner(d, z, m, x, rows):
        chunk = next(n for n, layers in enumerate(chunks) if x in layers)
        start, width = next((s, c) for k, at, s, c in zcols[chunk][z] if (k, at) == (m, x))
        count = abs(SPEEDS[m][1])
        shift = (start if z == 0 else start + width) % nz
        tile = zd[d, chunk, z]
        moved = pltpu.roll(tile, nz - shift, 1) if shift else tile
        moved = moved[TILE - count :] if d == 0 else moved[:count]
        line = lane[:count]
        return jnp.where(line < width if z == 0 else line >= nz - width, moved, rows)

    def crosses(m, x):
        return crossing(m, x, nx) is not None

    def stays(m, x):
        return crossing(m, x, nx) is None

    blank = jnp.zeros((ny, nz), jnp.float32)
    for chunk, layers in enumerate(chunks):
        packed = [blank, blank]
        for n, x in enumerate(layers):
            if chunk < 2:
                loads[2 * chunk + n].wait()
            elif n == 0:
                loads[4].wait()
            if x == order[0]:
                loads[5].wait()

            def between(x=x):
                if x == order[0]:
                    await_ready(0)
                send_edge(x)

            work(x, chunk, packed, between)
        for d in (0, 1):
            zs[chunk, d] = packed[d]
        if chunk == 0:
            await_ready(2)
            send_z(0)
            await_ready(1, 0)
            send_corners(0, 1, 0)
            pl.when(above[1][1] == 0)(lambda: send_corners(0, 1, 1))
        else:
            send_z(chunk)
        if chunk == 1:
            pack_y(0)
            send_y(0, 0)
            pl.when(above[1][1] == 0)(lambda: send_y(0, 1))
            pack_y(1)
            send_y(1, 0)
            pl.when(above[1][1] == 0)(lambda: send_y(1, 1))
    pack_y(2)
    send_y(2, 0)
    send_corners(1, 2, 0)

    def down_early():
        send_y(2, 1)
        send_corners(1, 2, 1)

    pl.when(above[1][1] == 0)(down_early)

    def wait_z(chunk):
        remote(((2, 0),), zs.at[chunk], zr.at[chunk], z_ss.at[0], z_rs.at[chunk]).wait_recv()

    wait_z(0)
    settle_z(0, crosses)
    for x in chunks[0]:
        send_tilted(x)
    wait_z(1)
    settle_z(1, crosses)
    for x in chunks[1]:
        send_tilted(x)

    def down_late():
        await_ready(1, 1)
        send_corners(0, 1, 1)
        send_y(0, 1)
        send_corners(1, 2, 1)
        send_y(1, 1)
        send_y(2, 1)

    pl.when(above[1][1] == 1)(down_late)
    settle_z(0, stays)
    settle_z(1, stays)

    def wait_y(kind):
        _, first, size = yrows[kind]
        part = (slice(None), pl.ds(first, size))
        remote(((1, 0),), ys.at[part], yr.at[part], y_ss.at[0], y_rs.at[kind]).wait_recv()

    def wait_corners(first, count):
        part = zd.at[:, pl.ds(first, count)]
        remote(((1, 0),), part, part, d_ss.at[0], d_rs.at[min(first, 1)]).wait_recv()

    wait_y(0)
    settle_y(0, lambda m, x: SPEEDS[m][2] == 0)
    for x in order:
        send_late(x, 0)
    wait_corners(0, 1)
    settle_y(0, lambda m, x: SPEEDS[m][2] != 0)
    for x in order:
        send_late(x, 1)
    wait_z(2)
    settle_z(2, stays)
    wait_corners(1, 2)
    wait_y(1)
    settle_y(1, stays)
    wait_y(2)
    settle_y(2, stays)
    units = sum(sent) // ny
    layers = max(n for n in range(1, nx + 1) if units % n == 0)
    span = ext.at[pl.ds(0, units // layers), pl.ds(0, layers), pl.ds(PY, ny)]
    everything = remote(((0, 0),), span, span, x_ss.at[0], x_rs.at[0])
    everything.wait_recv()
    everything.wait_send()
    remote(((1, 0),), ys, ys, y_ss.at[0], y_rs.at[0]).wait_send()
    remote(((1, 0),), zd, zd, d_ss.at[0], d_rs.at[0]).wait_send()
    remote(((2, 0),), zs, zs, z_ss.at[0], z_rs.at[0]).wait_send()


def crop(ext, out, sem):
    nx, ny = out.shape[1:3]
    inside = ext.at[:, pl.ds(PX, nx), pl.ds(PY, ny)]
    for m in range(Q):
        for x in range(nx):
            pltpu.make_async_copy(inside.at[m, x], out.at[m, x], sem).start()
    pltpu.make_async_copy(inside, out, sem).wait()


def per_device(populations, relax):
    nx, ny, nz = relax.shape
    shape = (Q, nx + 2 * PX, ny + 2 * PY, nz)
    height = plan(nx)[4]
    f32 = jnp.float32
    dma = pltpu.SemaphoreType.DMA
    any_space = pl.BlockSpec(memory_space=pl.ANY)
    room = 67043328 - 4 * math.prod(shape) - 32768
    ext = pl.pallas_call(
        kernel,
        out_shape=pltpu.VMEM(shape, f32),
        in_specs=[pl.BlockSpec(memory_space=pltpu.HBM)] * 2,
        out_specs=pl.BlockSpec(memory_space=pltpu.VMEM),
        scratch_shapes=[
            pltpu.VMEM((Q, nx, ny, nz), f32),
            pltpu.VMEM((nx, ny, nz), f32),
            pltpu.VMEM((3, 2, ny, nz), f32),
            pltpu.VMEM((3, 2, ny, nz), f32),
            pltpu.VMEM((2, 3, 2, TILE, nz), f32),
            pltpu.VMEM((2, height, nz), f32),
            pltpu.VMEM((2, height, nz), f32),
            dma((6,)),
            dma((1,)), dma((3,)),
            dma((1,)), dma((2,)),
            dma((1,)), dma((3,)),
            dma((1,)), dma((1,)),
            pltpu.SemaphoreType.REGULAR((4,)),
        ],
        compiler_params=pltpu.CompilerParams(
            collective_id=0, has_side_effects=True, vmem_limit_bytes=room
        ),
    )(populations, relax)
    return pl.pallas_call(
        crop,
        out_shape=jax.ShapeDtypeStruct((Q, nx, ny, nz), f32),
        in_specs=[any_space],
        out_specs=any_space,
        scratch_shapes=[dma],
        compiler_params=pltpu.CompilerParams(vmem_limit_bytes=2**20),
    )(ext)


def solution(mesh):
    return jax.shard_map(
        per_device,
        mesh=mesh,
        in_specs=(P(None, "gx", "gy", "gz"), P("gx", "gy", "gz")),
        out_specs=P(None, "gx", "gy", "gz"),
        check_vma=False,
    )
```

```python
import math

import jax
import jax.numpy as jnp
from jax import lax
from jax.experimental import pallas as pl
from jax.experimental.pallas import tpu as pltpu
from jax.sharding import PartitionSpec as P

MESH = pl.DeviceIdType.MESH
AXES = ("gx", "gy", "gz")
PX = 3
PY = 8
TILE = 8
FERRY = (2, 1)


def lattice():
    speeds = [(0, 0, 0)]
    weights = [1.0 / 12.0]
    for axis in range(3):
        for sign in (1, -1):
            vector = [0, 0, 0]
            vector[axis] = sign
            speeds.append(tuple(vector))
            weights.append(1.0 / 12.0)
    for first in (1, -1):
        for second in (1, -1):
            for third in (1, -1):
                speeds.append((first, second, third))
                weights.append(1.0 / 27.0)
    for axis in range(3):
        for sign in (2, -2):
            vector = [0, 0, 0]
            vector[axis] = sign
            speeds.append(tuple(vector))
            weights.append(2.0 / 135.0)
    for couple in ((0, 1), (0, 2), (1, 2)):
        for first in (2, -2):
            for second in (2, -2):
                vector = [0, 0, 0]
                vector[couple[0]] = first
                vector[couple[1]] = second
                speeds.append(tuple(vector))
                weights.append(1.0 / 432.0)
    for axis in range(3):
        for sign in (3, -3):
            vector = [0, 0, 0]
            vector[axis] = sign
            speeds.append(tuple(vector))
            weights.append(1.0 / 1620.0)
    return (speeds, weights)


SPEEDS, WEIGHTS = lattice()
Q = len(SPEEDS)
SQUARES = [sum(v * v for v in c) for c in SPEEDS]
PAIRS = [
    (m, SPEEDS.index(tuple(-v for v in SPEEDS[m])))
    for m in range(1, Q)
    if m < SPEEDS.index(tuple(-v for v in SPEEDS[m]))
]


EDGE = [
    (m, o) for m, o in PAIRS if SPEEDS[m][2] == 0 and SPEEDS[m][0] != 0
]
REST = [pair for pair in PAIRS if pair not in EDGE]


def crossing(m, x, nx):
    at = x + SPEEDS[m][0]
    return 0 if at >= nx else 1 if at < 0 else None


def slots(axis, sign, layers, keep):
    rows, start = [], 0
    for x in layers:
        for m, c in enumerate(SPEEDS):
            count = c[axis] * sign
            if count > 0 and keep(m, x):
                rows.append((m, x, start, count))
                start += count
    return rows, start


def plan(nx):
    order = []
    for x in range((nx + 1) // 2):
        order += [x] if x == nx - 1 - x else [x, nx - 1 - x]
    chunks = [order[:2], order[2:4], order[4:]]
    zcols = [
        [slots(2, sign, layers, lambda m, x: True)[0] for sign in (1, -1)]
        for layers in chunks
    ]
    near = set(order[:4])
    kinds = [
        lambda m, x: crossing(m, x, nx) is not None,
        lambda m, x: crossing(m, x, nx) is None and x in near,
        lambda m, x: crossing(m, x, nx) is None and x not in near,
    ]
    yrows, start = [], 0
    for keep in kinds:
        both = [slots(1, sign, order, keep) for sign in (1, -1)]
        size = -(-max(n for _, n in both) // TILE) * TILE
        yrows.append(([rows for rows, _ in both], start, size))
        start += size
    return order, chunks, zcols, yrows, start


def add_all(terms):
    total = terms[0]
    for term in terms[1:]:
        total = total + term
    return total


def collide(load, rate):
    sums = {k: [] for k in (1, 3, 4, 8, 9)}
    flows = {k: [[], [], []] for k in (1, 3, 4, 8, 9)}
    for m, o in PAIRS:
        up, down = load(m), load(o)
        k = SQUARES[m]
        sums[k].append(up + down)
        diff = up - down
        for axis in range(3):
            if SPEEDS[m][axis] > 0:
                flows[k][axis].append((1, diff))
            elif SPEEDS[m][axis] < 0:
                flows[k][axis].append((-1, diff))
    weight = {SQUARES[m]: WEIGHTS[m] for m in range(Q)}
    size = {1: 1, 3: 1, 4: 2, 8: 2, 9: 3}
    rest = load(0)
    groups = {k: add_all(sums[k]) for k in sums}
    rho = weight[0] * rest
    energy = None
    for k in sums:
        part = weight[k] * groups[k]
        rho = rho + part
        part = part if k == 1 else float(k) * part
        energy = part if energy is None else energy + part
    flux = []
    for axis in range(3):
        total = None
        for k in flows:
            part = None
            for sign, diff in flows[k][axis]:
                if part is None:
                    part = diff if sign > 0 else -diff
                else:
                    part = part + diff if sign > 0 else part - diff
            part = (weight[k] * size[k]) * part
            total = part if total is None else total + part
        flux.append(total)
    inverse = 1.0 / rho
    velocity = [part * inverse for part in flux]
    norm = velocity[0] * velocity[0] + velocity[1] * velocity[1] + velocity[2] * velocity[2]
    t = (energy * inverse - norm) * 0.5 - 1.0
    b = 1.5 * norm
    w = [1.5 * part for part in velocity]
    keep = 1.0 - rate
    k0 = rho * rate
    k24 = k0 * (1.0 / 24.0)
    k6 = k0 * (1.0 / 6.0)
    half_b = 0.5 * b
    kt = k0 * t
    ktb = kt * b
    ktt = kt * t
    base = k0 * (1.0 - half_b + 0.5 * half_b * half_b)
    base1 = k0 * (0.5 - 0.5 * half_b)
    baseo = k0 * (1.0 - half_b)

    def even0(s):
        return (
            base
            + kt * (0.5 * (s - 3.0))
            + ktb * (0.25 * (5.0 - s))
            + ktt * ((s * s - 10.0 * s + 15.0) / 8.0)
        )

    def emit_rest(emit):
        emit(0, keep * rest + even0(0.0))

    def emit_pairs(pairs, emit):
        for k in sums:
            chosen = [pair for pair in pairs if SQUARES[pair[0]] == k]
            if not chosen:
                continue
            s = 1.5 * k
            e0 = even0(s)
            e1 = base1 + kt * (0.25 * (s - 7.0))
            o1 = baseo + kt * (0.5 * (s - 5.0))
            for m, o in chosen:
                a = None
                for axis in range(3):
                    v = SPEEDS[m][axis]
                    if v == 0:
                        continue
                    unit = w[axis]
                    if a is None:
                        a = unit if v > 0 else -unit
                    else:
                        a = a + unit if v > 0 else a - unit
                if size[k] != 1:
                    a = float(size[k]) * a
                q = a * a
                even = e0 + q * (e1 + q * k24)
                odd = a * (o1 + q * k6)
                emit(m, keep * load(m) + (even + odd))
                emit(o, keep * load(o) + (even - odd))

    return emit_rest, emit_pairs


def kernel(
    pop, rate, ext, g, r, zs, zr, zd, ys, yr, hop,
    in_sem, z_ss, z_rs, d_ss, d_rs, y_ss, y_rs, x_ss, x_rs, h_ss, h_rs, ready,
):
    nx, ny, nz = pop.shape[1:]
    order, chunks, zcols, yrows, _ = plan(nx)
    groups = [(x, 1) for x in order[:4]] + [(2, nx - 4)]
    loads = [
        pltpu.make_async_copy(
            pop.at[:, pl.ds(first, count)], g.at[:, pl.ds(first, count)], in_sem.at[n]
        )
        for n, (first, count) in enumerate(groups)
    ]
    loads.append(pltpu.make_async_copy(rate, r, in_sem.at[5]))

    around, above, nears = [], [], []
    for axis in AXES:
        n = lax.axis_size(axis)
        me = lax.axis_index(axis)
        near = (lax.rem(me + 1, n), lax.rem(me + n - 1, n))
        nears.append(near)
        around.append(tuple({axis: at} for at in near))
        above.append(tuple(jnp.where(at > me, 1, 0) for at in near))
    barrier = pltpu.get_barrier_semaphore()

    links = [
        (((0, d),), 0) for d in (0, 1)
    ] + [
        (((2, d),), 1) for d in (0, 1)
    ] + [
        (((1, d), (2, z))[: 1 if z is None else 2], 2 + d)
        for d in (0, 1) for z in (None, 0, 1)
    ]

    def at(steps):
        return {name: v for axis, d in steps for name, v in around[axis][d].items()}

    size = [lax.axis_size(axis) for axis in AXES]
    me = [lax.axis_index(axis) for axis in AXES]
    last = [jnp.where(me[1] == end, 1, 0) for end in (size[1] - 1, 0)]
    chip = me[2] // 2
    apart = [
        jnp.where((n // 2 != chip) & (jnp.maximum(n, me[2]) - jnp.minimum(n, me[2]) == 1), 1, 0)
        for n in nears[2]
    ]

    def is_above(steps):
        (axis, d), z = steps[0], steps[-1][1]
        if len(steps) == 1:
            return above[axis][d]
        aside = (1 - last[d]) * apart[z]
        return (1 - aside) * above[axis][d] + aside * above[2][z]

    def signal(semaphore, steps):
        pl.semaphore_signal(semaphore, inc=1, device_id=at(steps), device_id_type=MESH)

    def wait(semaphore, amount):
        pl.when(amount > 0)(lambda: pl.semaphore_wait(semaphore, amount))

    ferry = [
        [(SPEEDS.index((PX, 0, 0)), nx - 1 - n) for n in range(FERRY[0])],
        [(SPEEDS.index((-PX, 0, 0)), n) for n in range(FERRY[1])],
    ]
    into = [jnp.where((nears[0][d] == 0) & (me[1] == 0), 1, 0) for d in (0, 1)]
    source = [jnp.where(chip == 0, into[d], 0) for d in (0, 1)]
    carrier = [jnp.where(chip == 1, into[d], 0) for d in (0, 1)]
    final = jnp.where((me[0] == 0) & (me[1] == 0) & (chip == 0), 1, 0)
    beyond = {AXES[2]: lax.rem(me[2] + 2, size[2])}
    before = {AXES[2]: lax.rem(me[2] + size[2] - 2, size[2])}

    def signal_to(semaphore, target):
        pl.semaphore_signal(semaphore, inc=1, device_id=target, device_id_type=MESH)

    for steps, _ in links:
        pl.when(is_above(steps) == 1)(lambda p=steps: signal(barrier, p))
    for d in (0, 1):
        pl.when(source[d] == 1)(lambda: signal_to(barrier, beyond))
        pl.when(final == 1)(lambda d=d: signal_to(barrier, {**around[0][1 - d], **beyond}))
    for n in (0, 5, 1, 2, 3, 4):
        loads[n].start()
    wait(
        barrier,
        sum(1 - is_above(steps) for steps, _ in links) + 2 * (carrier[0] + carrier[1]),
    )
    for steps, flag in links:
        back = 5 - flag if flag > 1 else flag
        pl.when(is_above(steps) == 0)(lambda p=steps, f=back: signal(ready.at[f], p))
    for d in (0, 1):
        pl.when(carrier[d] == 1)(lambda: signal_to(ready.at[4], before))

    def await_ready(axis, d=None):
        flag = 2 + d if axis == 1 else axis // 2
        wait(ready.at[flag], sum(is_above(steps) for steps, f in links if f == flag))

    lane = lax.broadcasted_iota(jnp.int32, (ny, nz), 1)

    def rows_at(m):
        return pl.ds(PY + SPEEDS[m][1], ny)

    def place(m, x):
        return PX + x + SPEEDS[m][0]

    def remote(steps, src, dst, ss, rs):
        return pltpu.make_async_remote_copy(
            src_ref=src, dst_ref=dst, send_sem=ss, recv_sem=rs,
            device_id=at(steps), device_id_type=MESH,
        )

    def x_copy(m, members, x, rows):
        d = crossing(m, x, nx)
        at_x = place(m, x)
        home = at_x - nx if d == 0 else at_x + nx
        which, rows = pl.ds(m, members), pl.ds(PY + rows[0], rows[1])
        return remote(
            ((0, d),), ext.at[which, pl.ds(at_x, 1), rows], ext.at[which, pl.ds(home, 1), rows],
            x_ss.at[0], x_rs.at[0],
        )

    def send_x(m, members, x, rows):
        copy = x_copy(m, members, x, rows)
        d = crossing(m, x, nx)
        if (m, x) in ferry[d]:
            pl.when(source[d] == 0)(copy.start)
        else:
            copy.start()

    def board(d):
        for n, (m, x) in enumerate(ferry[d]):
            pltpu.make_async_remote_copy(
                src_ref=ext.at[m, place(m, x), pl.ds(PY, ny)], dst_ref=hop.at[d, n],
                send_sem=x_ss.at[0], recv_sem=h_rs.at[d],
                device_id=beyond, device_id_type=MESH,
            ).start()

    def carry(d):
        span = hop.at[d, pl.ds(0, len(ferry[d]))]
        landed = remote(((2, 0),), span, span, h_ss.at[d], h_rs.at[d])
        landed.wait_recv()
        for n, (m, x) in enumerate(ferry[d]):
            at_x = place(m, x)
            home = at_x - nx if d == 0 else at_x + nx
            pltpu.make_async_remote_copy(
                src_ref=hop.at[d, n], dst_ref=ext.at[m, home, pl.ds(PY, ny)],
                send_sem=h_ss.at[d], recv_sem=x_rs.at[0],
                device_id={**around[0][d], **before}, device_id_type=MESH,
            ).start()

    def carried(d):
        span = hop.at[d, pl.ds(0, len(ferry[d]))]
        remote(((2, 0),), span, span, h_ss.at[d], h_rs.at[d]).wait_send()

    def ferry_when(role, act):
        for d in (0, 1):
            if ferry[d]:
                pl.when(role[d] == 1)(lambda d=d: act(d))

    def send_z(chunk):
        for d in (0, 1):
            remote(
                ((2, d),), zs.at[chunk, d], zr.at[chunk, d], z_ss.at[0], z_rs.at[chunk]
            ).start()

    def send_corners(first, count, d):
        part = pl.ds(first, count)
        rows = pl.ds(ny - TILE if d == 0 else 0, TILE)
        for z in (0, 1):
            remote(
                ((1, d), (2, z)), zs.at[part, z, rows], zd.at[d, part, z],
                d_ss.at[0], d_rs.at[first // 2],
            ).start()

    def send_y(kind, d):
        _, start, size = yrows[kind]
        rows = pl.ds(start, size)
        remote(
            ((1, d),), ys.at[d, rows], yr.at[d, rows], y_ss.at[0], y_rs.at[kind]
        ).start()

    def first_down():
        await_ready(1, 1)
        send_corners(0, 2, 1)
        send_y(0, 1)

    def early(m):
        v = SPEEDS[m][1]
        return (0, ny) if v == 0 else (TILE, ny - TILE) if v > 0 else (0, ny - TILE)

    def late(m):
        return (0, TILE) if SPEEDS[m][1] > 0 else (ny - TILE, TILE)

    def outgoing(x, chosen):
        return [m for m in range(Q) if crossing(m, x, nx) is not None and chosen(SPEEDS[m])]

    def send_edge(x):
        for m in outgoing(x, lambda c: c[2] == 0):
            send_x(m, 1, x, early(m))

    def send_tilted(x):
        for m in outgoing(x, lambda c: c[2] > 0):
            send_x(m, 2, x, early(m))

    def send_late(x, tilted):
        for m in outgoing(x, lambda c: c[1] != 0 and (c[2] > 0 if tilted else c[2] == 0)):
            send_x(m, 1 + tilted, x, late(m))

    def work(x, chunk, packed, between):
        slot = [{m: (s, c) for m, at, s, c in zcols[chunk][d] if at == x} for d in (0, 1)]

        def emit(m, value):
            cz = SPEEDS[m][2]
            if cz:
                d = 0 if cz > 0 else 1
                start, count = slot[d][m]
                shift = (start + count if d == 0 else start) % nz
                moved = pltpu.roll(value, shift, 1) if shift else value
                mask = (lane >= start) & (lane < start + count)
                packed[d] = jnp.where(mask, moved, packed[d])
                value = pltpu.roll(value, cz % nz, 1)
            ext[m, place(m, x), rows_at(m), :] = value

        emit_rest, emit_pairs = collide(lambda m: g[m, x], r[x])
        emit_pairs(EDGE, emit)
        between()
        emit_rest(emit)
        emit_pairs(REST, emit)

    def settle_z(chunk, chosen):
        for d in (0, 1):
            base = zr[chunk, d]
            for m, x, start, count in zcols[chunk][d]:
                if not chosen(m, x):
                    continue
                shift = (start if d == 0 else start + count) % nz
                moved = pltpu.roll(base, nz - shift, 1) if shift else base
                mask = lane < count if d == 0 else lane >= nz - count
                where = (m, place(m, x), rows_at(m), slice(None))
                ext[where] = jnp.where(mask, moved, ext[where])

    def pack_y(kind):
        tables, first, _ = yrows[kind]
        for d in (0, 1):
            for m, x, start, count in tables[d]:
                edge = PY + ny if d == 0 else PY - count
                ys[d, pl.ds(first + start, count), :] = ext[
                    m, place(m, x), pl.ds(edge, count), :
                ]

    def settle_y(kind, chosen):
        tables, first, _ = yrows[kind]
        for d in (0, 1):
            for m, x, start, count in tables[d]:
                if not chosen(m, x):
                    continue
                home = PY if d == 0 else PY + ny - count
                rows = yr[d, pl.ds(first + start, count), :]
                cz = SPEEDS[m][2]
                if cz:
                    z = 0 if cz > 0 else 1
                    rows = corner(d, z, m, x, rows)
                ext[m, place(m, x), pl.ds(home, count), :] = rows

    def corner(d, z, m, x, rows):
        chunk = next(n for n, layers in enumerate(chunks) if x in layers)
        start, width = next((s, c) for k, at, s, c in zcols[chunk][z] if (k, at) == (m, x))
        count = abs(SPEEDS[m][1])
        shift = (start if z == 0 else start + width) % nz
        tile = zd[d, chunk, z]
        moved = pltpu.roll(tile, nz - shift, 1) if shift else tile
        moved = moved[TILE - count :] if d == 0 else moved[:count]
        line = lane[:count]
        return jnp.where(line < width if z == 0 else line >= nz - width, moved, rows)

    def crosses(m, x):
        return crossing(m, x, nx) is not None

    def stays(m, x):
        return crossing(m, x, nx) is None

    blank = jnp.zeros((ny, nz), jnp.float32)
    for chunk, layers in enumerate(chunks):
        packed = [blank, blank]
        for n, x in enumerate(layers):
            if chunk < 2:
                loads[2 * chunk + n].wait()
            elif n == 0:
                loads[4].wait()
            if x == order[0]:
                loads[5].wait()

            def between(x=x):
                if x == order[0]:
                    await_ready(0)
                send_edge(x)

            work(x, chunk, packed, between)
        for d in (0, 1):
            zs[chunk, d] = packed[d]
        if chunk == 0:
            await_ready(2)
        send_z(chunk)
        if chunk == 1:
            wait(ready.at[4], source[0] + source[1])
            ferry_when(source, board)
            pack_y(0)
            pack_y(1)
            await_ready(1, 0)
            send_corners(0, 2, 0)
            send_y(0, 0)
            send_y(1, 0)
            pl.when(above[1][1] == 0)(first_down)
    pack_y(2)
    send_y(2, 0)
    send_corners(2, 1, 0)

    def wait_z(chunk):
        remote(((2, 0),), zs.at[chunk], zr.at[chunk], z_ss.at[0], z_rs.at[chunk]).wait_recv()

    ferry_when(carrier, carry)
    wait_z(0)
    settle_z(0, crosses)
    for x in chunks[0]:
        send_tilted(x)
    wait_z(1)
    settle_z(1, crosses)
    for x in chunks[1]:
        send_tilted(x)

    pl.when(above[1][1] == 1)(first_down)
    send_y(1, 1)
    send_y(2, 1)
    send_corners(2, 1, 1)
    settle_z(0, stays)
    settle_z(1, stays)

    def wait_y(kind):
        _, first, size = yrows[kind]
        part = (slice(None), pl.ds(first, size))
        remote(((1, 0),), ys.at[part], yr.at[part], y_ss.at[0], y_rs.at[kind]).wait_recv()

    def wait_corners(first, count):
        part = zd.at[:, pl.ds(first, count)]
        remote(((1, 0),), part, part, d_ss.at[0], d_rs.at[first // 2]).wait_recv()

    wait_y(0)
    settle_y(0, lambda m, x: SPEEDS[m][2] == 0)
    for x in order:
        send_late(x, 0)
    wait_corners(0, 2)
    settle_y(0, lambda m, x: SPEEDS[m][2] != 0)
    for x in order:
        send_late(x, 1)
    wait_z(2)
    settle_z(2, stays)
    wait_corners(2, 1)
    wait_y(1)
    settle_y(1, stays)
    wait_y(2)
    settle_y(2, stays)
    units = sum(abs(c[0]) for c in SPEEDS)
    layers = max(n for n in range(1, nx + 1) if units % n == 0)
    span = ext.at[pl.ds(0, units // layers), pl.ds(0, layers), pl.ds(PY, ny)]
    everything = remote(((0, 0),), span, span, x_ss.at[0], x_rs.at[0])
    everything.wait_recv()
    everything.wait_send()
    ferry_when(carrier, carried)
    remote(((1, 0),), ys, ys, y_ss.at[0], y_rs.at[0]).wait_send()
    remote(((1, 0),), zd, zd, d_ss.at[0], d_rs.at[0]).wait_send()
    remote(((2, 0),), zs, zs, z_ss.at[0], z_rs.at[0]).wait_send()


def crop(ext, out, sem):
    nx, ny = out.shape[1:3]
    inside = ext.at[:, pl.ds(PX, nx), pl.ds(PY, ny)]
    for m in range(Q):
        for x in range(nx):
            pltpu.make_async_copy(inside.at[m, x], out.at[m, x], sem).start()
    pltpu.make_async_copy(inside, out, sem).wait()


def per_device(populations, relax):
    nx, ny, nz = relax.shape
    shape = (Q, nx + 2 * PX, ny + 2 * PY, nz)
    height = plan(nx)[4]
    f32 = jnp.float32
    dma = pltpu.SemaphoreType.DMA
    any_space = pl.BlockSpec(memory_space=pl.ANY)
    room = 67043328 - 4 * math.prod(shape) - 32768
    ext = pl.pallas_call(
        kernel,
        out_shape=pltpu.VMEM(shape, f32),
        in_specs=[pl.BlockSpec(memory_space=pltpu.HBM)] * 2,
        out_specs=pl.BlockSpec(memory_space=pltpu.VMEM),
        scratch_shapes=[
            pltpu.VMEM((Q, nx, ny, nz), f32),
            pltpu.VMEM((nx, ny, nz), f32),
            pltpu.VMEM((3, 2, ny, nz), f32),
            pltpu.VMEM((3, 2, ny, nz), f32),
            pltpu.VMEM((2, 3, 2, TILE, nz), f32),
            pltpu.VMEM((2, height, nz), f32),
            pltpu.VMEM((2, height, nz), f32),
            pltpu.VMEM((2, max(1, *FERRY), ny, nz), f32),
            dma((6,)),
            dma((1,)), dma((3,)),
            dma((1,)), dma((2,)),
            dma((1,)), dma((3,)),
            dma((1,)), dma((1,)),
            dma((2,)), dma((2,)),
            pltpu.SemaphoreType.REGULAR((5,)),
        ],
        compiler_params=pltpu.CompilerParams(
            collective_id=0, has_side_effects=True, vmem_limit_bytes=room
        ),
    )(populations, relax)
    return pl.pallas_call(
        crop,
        out_shape=jax.ShapeDtypeStruct((Q, nx, ny, nz), f32),
        in_specs=[any_space],
        out_specs=any_space,
        scratch_shapes=[dma],
        compiler_params=pltpu.CompilerParams(vmem_limit_bytes=2**20),
    )(ext)


def solution(mesh):
    return jax.shard_map(
        per_device,
        mesh=mesh,
        in_specs=(P(None, "gx", "gy", "gz"), P("gx", "gy", "gz")),
        out_specs=P(None, "gx", "gy", "gz"),
        check_vma=False,
    )
```

```python
import math

import jax
import jax.numpy as jnp
from jax import lax
from jax.experimental import pallas as pl
from jax.experimental.pallas import tpu as pltpu
from jax.sharding import PartitionSpec as P

MESH = pl.DeviceIdType.MESH
AXES = ("gx", "gy", "gz")
PX = 3
PY = 8
TILE = 8
CORNER = 2
FERRY = (2, 1)


def lattice():
    speeds = [(0, 0, 0)]
    weights = [1.0 / 12.0]
    for axis in range(3):
        for sign in (1, -1):
            vector = [0, 0, 0]
            vector[axis] = sign
            speeds.append(tuple(vector))
            weights.append(1.0 / 12.0)
    for first in (1, -1):
        for second in (1, -1):
            for third in (1, -1):
                speeds.append((first, second, third))
                weights.append(1.0 / 27.0)
    for axis in range(3):
        for sign in (2, -2):
            vector = [0, 0, 0]
            vector[axis] = sign
            speeds.append(tuple(vector))
            weights.append(2.0 / 135.0)
    for couple in ((0, 1), (0, 2), (1, 2)):
        for first in (2, -2):
            for second in (2, -2):
                vector = [0, 0, 0]
                vector[couple[0]] = first
                vector[couple[1]] = second
                speeds.append(tuple(vector))
                weights.append(1.0 / 432.0)
    for axis in range(3):
        for sign in (3, -3):
            vector = [0, 0, 0]
            vector[axis] = sign
            speeds.append(tuple(vector))
            weights.append(1.0 / 1620.0)
    return (speeds, weights)


SPEEDS, WEIGHTS = lattice()
Q = len(SPEEDS)
SQUARES = [sum(v * v for v in c) for c in SPEEDS]
PAIRS = [
    (m, SPEEDS.index(tuple(-v for v in SPEEDS[m])))
    for m in range(1, Q)
    if m < SPEEDS.index(tuple(-v for v in SPEEDS[m]))
]


EDGE = [
    (m, o) for m, o in PAIRS if SPEEDS[m][2] == 0 and SPEEDS[m][0] != 0
]
REST = [pair for pair in PAIRS if pair not in EDGE]


def crossing(m, x, nx):
    at = x + SPEEDS[m][0]
    return 0 if at >= nx else 1 if at < 0 else None


def slots(axis, sign, layers, keep):
    rows, start = [], 0
    for x in layers:
        for m, c in enumerate(SPEEDS):
            count = c[axis] * sign
            if count > 0 and keep(m, x):
                rows.append((m, x, start, count))
                start += count
    return rows, start


def plan(nx):
    order = []
    for x in range((nx + 1) // 2):
        order += [x] if x == nx - 1 - x else [x, nx - 1 - x]
    chunks = [order[:2], order[2:4], order[4:]]
    zcols = [
        [slots(2, sign, layers, lambda m, x: True)[0] for sign in (1, -1)]
        for layers in chunks
    ]
    stages = chunks[:2] + [order[4:6], order[6:]]
    yrows, start = [], 0
    kinds = [(order, True)] + [(layers, False) for layers in stages]
    for layers, out in kinds:
        both = [
            slots(1, sign, layers, lambda m, x: (crossing(m, x, nx) is not None) == out)
            for sign in (1, -1)
        ]
        size = -(-max(n for _, n in both) // TILE) * TILE
        yrows.append(([rows for rows, _ in both], start, size))
        start += size
    return order, chunks, zcols, yrows, start


def add_all(terms):
    total = terms[0]
    for term in terms[1:]:
        total = total + term
    return total


def collide(load, rate):
    sums = {k: [] for k in (1, 3, 4, 8, 9)}
    flows = {k: [[], [], []] for k in (1, 3, 4, 8, 9)}
    for m, o in PAIRS:
        up, down = load(m), load(o)
        k = SQUARES[m]
        sums[k].append(up + down)
        diff = up - down
        for axis in range(3):
            if SPEEDS[m][axis] > 0:
                flows[k][axis].append((1, diff))
            elif SPEEDS[m][axis] < 0:
                flows[k][axis].append((-1, diff))
    weight = {SQUARES[m]: WEIGHTS[m] for m in range(Q)}
    size = {1: 1, 3: 1, 4: 2, 8: 2, 9: 3}
    rest = load(0)
    groups = {k: add_all(sums[k]) for k in sums}
    rho = weight[0] * rest
    energy = None
    for k in sums:
        part = weight[k] * groups[k]
        rho = rho + part
        part = part if k == 1 else float(k) * part
        energy = part if energy is None else energy + part
    flux = []
    for axis in range(3):
        total = None
        for k in flows:
            part = None
            for sign, diff in flows[k][axis]:
                if part is None:
                    part = diff if sign > 0 else -diff
                else:
                    part = part + diff if sign > 0 else part - diff
            part = (weight[k] * size[k]) * part
            total = part if total is None else total + part
        flux.append(total)
    inverse = 1.0 / rho
    velocity = [part * inverse for part in flux]
    norm = velocity[0] * velocity[0] + velocity[1] * velocity[1] + velocity[2] * velocity[2]
    t = (energy * inverse - norm) * 0.5 - 1.0
    b = 1.5 * norm
    w = [1.5 * part for part in velocity]
    keep = 1.0 - rate
    k0 = rho * rate
    k24 = k0 * (1.0 / 24.0)
    k6 = k0 * (1.0 / 6.0)
    half_b = 0.5 * b
    kt = k0 * t
    ktb = kt * b
    ktt = kt * t
    base = k0 * (1.0 - half_b + 0.5 * half_b * half_b)
    base1 = k0 * (0.5 - 0.5 * half_b)
    baseo = k0 * (1.0 - half_b)

    def even0(s):
        return (
            base
            + kt * (0.5 * (s - 3.0))
            + ktb * (0.25 * (5.0 - s))
            + ktt * ((s * s - 10.0 * s + 15.0) / 8.0)
        )

    def emit_rest(emit):
        emit(0, keep * rest + even0(0.0))

    def emit_pairs(pairs, emit):
        for k in sums:
            chosen = [pair for pair in pairs if SQUARES[pair[0]] == k]
            if not chosen:
                continue
            s = 1.5 * k
            e0 = even0(s)
            e1 = base1 + kt * (0.25 * (s - 7.0))
            o1 = baseo + kt * (0.5 * (s - 5.0))
            for m, o in chosen:
                a = None
                for axis in range(3):
                    v = SPEEDS[m][axis]
                    if v == 0:
                        continue
                    unit = w[axis]
                    if a is None:
                        a = unit if v > 0 else -unit
                    else:
                        a = a + unit if v > 0 else a - unit
                if size[k] != 1:
                    a = float(size[k]) * a
                q = a * a
                even = e0 + q * (e1 + q * k24)
                odd = a * (o1 + q * k6)
                emit(m, keep * load(m) + (even + odd))
                emit(o, keep * load(o) + (even - odd))

    return emit_rest, emit_pairs


def kernel(
    pop, rate, ext, g, r, zs, zr, zc, zd, ys, yr, hop,
    in_sem, z_ss, z_rs, d_ss, d_rs, y_ss, y_rs, x_ss, x_rs, h_ss, h_rs, ready,
):
    nx, ny, nz = pop.shape[1:]
    order, chunks, zcols, yrows, _ = plan(nx)
    groups = [(x, 1) for x in order[:4]] + [(2, nx - 4)]
    loads = [
        pltpu.make_async_copy(
            pop.at[:, pl.ds(first, count)], g.at[:, pl.ds(first, count)], in_sem.at[n]
        )
        for n, (first, count) in enumerate(groups)
    ]
    loads.append(pltpu.make_async_copy(rate, r, in_sem.at[5]))

    around, above, nears = [], [], []
    for axis in AXES:
        n = lax.axis_size(axis)
        me = lax.axis_index(axis)
        near = (lax.rem(me + 1, n), lax.rem(me + n - 1, n))
        nears.append(near)
        around.append(tuple({axis: at} for at in near))
        above.append(tuple(jnp.where(at > me, 1, 0) for at in near))
    barrier = pltpu.get_barrier_semaphore()

    links = [
        (((0, d),), 0) for d in (0, 1)
    ] + [
        (((2, d),), 1) for d in (0, 1)
    ] + [
        (((1, d), (2, z))[: 1 if z is None else 2], 2 + d)
        for d in (0, 1) for z in (None, 0, 1)
    ]

    def at(steps):
        return {name: v for axis, d in steps for name, v in around[axis][d].items()}

    size = [lax.axis_size(axis) for axis in AXES]
    me = [lax.axis_index(axis) for axis in AXES]
    last = [jnp.where(me[1] == end, 1, 0) for end in (size[1] - 1, 0)]
    chip = me[2] // 2
    apart = [
        jnp.where((n // 2 != chip) & (jnp.maximum(n, me[2]) - jnp.minimum(n, me[2]) == 1), 1, 0)
        for n in nears[2]
    ]

    def is_above(steps):
        (axis, d), z = steps[0], steps[-1][1]
        if len(steps) == 1:
            return above[axis][d]
        aside = (1 - last[d]) * apart[z]
        return (1 - aside) * above[axis][d] + aside * above[2][z]

    def signal(semaphore, steps):
        pl.semaphore_signal(semaphore, inc=1, device_id=at(steps), device_id_type=MESH)

    def wait(semaphore, amount):
        pl.when(amount > 0)(lambda: pl.semaphore_wait(semaphore, amount))

    ferry = [
        [(SPEEDS.index((PX, 0, 0)), nx - 1 - n) for n in range(FERRY[0])],
        [(SPEEDS.index((-PX, 0, 0)), n) for n in range(FERRY[1])],
    ]
    into = [jnp.where((nears[0][d] == 0) & (me[1] == 0), 1, 0) for d in (0, 1)]
    source = [jnp.where(chip == 0, into[d], 0) for d in (0, 1)]
    carrier = [jnp.where(chip == 1, into[d], 0) for d in (0, 1)]
    final = jnp.where((me[0] == 0) & (me[1] == 0) & (chip == 0), 1, 0)
    beyond = {AXES[2]: lax.rem(me[2] + 2, size[2])}
    before = {AXES[2]: lax.rem(me[2] + size[2] - 2, size[2])}

    def signal_to(semaphore, target):
        pl.semaphore_signal(semaphore, inc=1, device_id=target, device_id_type=MESH)

    for steps, _ in links:
        pl.when(is_above(steps) == 1)(lambda p=steps: signal(barrier, p))
    for d in (0, 1):
        pl.when(source[d] == 1)(lambda: signal_to(barrier, beyond))
        pl.when(final == 1)(lambda d=d: signal_to(barrier, {**around[0][1 - d], **beyond}))
    for n in (0, 5, 1, 2, 3, 4):
        loads[n].start()
    wait(
        barrier,
        sum(1 - is_above(steps) for steps, _ in links) + 2 * (carrier[0] + carrier[1]),
    )
    for steps, flag in links:
        back = 5 - flag if flag > 1 else flag
        pl.when(is_above(steps) == 0)(lambda p=steps, f=back: signal(ready.at[f], p))
    for d in (0, 1):
        pl.when(carrier[d] == 1)(lambda: signal_to(ready.at[4], before))

    def await_ready(axis, d=None):
        flag = 2 + d if axis == 1 else axis // 2
        wait(ready.at[flag], sum(is_above(steps) for steps, f in links if f == flag))

    lane = lax.broadcasted_iota(jnp.int32, (ny, nz), 1)

    def rows_at(m):
        return pl.ds(PY + SPEEDS[m][1], ny)

    def place(m, x):
        return PX + x + SPEEDS[m][0]

    def remote(steps, src, dst, ss, rs):
        return pltpu.make_async_remote_copy(
            src_ref=src, dst_ref=dst, send_sem=ss, recv_sem=rs,
            device_id=at(steps), device_id_type=MESH,
        )

    def x_copy(m, members, x, rows):
        d = crossing(m, x, nx)
        at_x = place(m, x)
        home = at_x - nx if d == 0 else at_x + nx
        which, rows = pl.ds(m, members), pl.ds(PY + rows[0], rows[1])
        return remote(
            ((0, d),), ext.at[which, pl.ds(at_x, 1), rows], ext.at[which, pl.ds(home, 1), rows],
            x_ss.at[0], x_rs.at[0],
        )

    def send_x(m, members, x, rows):
        copy = x_copy(m, members, x, rows)
        d = crossing(m, x, nx)
        if (m, x) in ferry[d]:
            pl.when(source[d] == 0)(copy.start)
        else:
            copy.start()

    def board(d):
        for n, (m, x) in enumerate(ferry[d]):
            pltpu.make_async_remote_copy(
                src_ref=ext.at[m, place(m, x), pl.ds(PY, ny)], dst_ref=hop.at[d, n],
                send_sem=x_ss.at[0], recv_sem=h_rs.at[d],
                device_id=beyond, device_id_type=MESH,
            ).start()

    def carry(d):
        span = hop.at[d, pl.ds(0, len(ferry[d]))]
        landed = remote(((2, 0),), span, span, h_ss.at[d], h_rs.at[d])
        landed.wait_recv()
        for n, (m, x) in enumerate(ferry[d]):
            at_x = place(m, x)
            home = at_x - nx if d == 0 else at_x + nx
            pltpu.make_async_remote_copy(
                src_ref=hop.at[d, n], dst_ref=ext.at[m, home, pl.ds(PY, ny)],
                send_sem=h_ss.at[d], recv_sem=x_rs.at[0],
                device_id={**around[0][d], **before}, device_id_type=MESH,
            ).start()

    def carried(d):
        span = hop.at[d, pl.ds(0, len(ferry[d]))]
        remote(((2, 0),), span, span, h_ss.at[d], h_rs.at[d]).wait_send()

    def ferry_when(role, act):
        for d in (0, 1):
            if ferry[d]:
                pl.when(role[d] == 1)(lambda d=d: act(d))

    def send_z(chunk):
        for d in (0, 1):
            remote(
                ((2, d),), zs.at[chunk, d], zr.at[chunk, d], z_ss.at[0], z_rs.at[chunk]
            ).start()

    def pack_corners(part):
        layers = (0,) if part == 0 else range(1, len(chunks))
        for d in (0, 1):
            first = ny - CORNER if d == 0 else 0
            for z in (0, 1):
                for n, chunk in enumerate(layers):
                    zc[part, d, z, pl.ds(CORNER * n, CORNER), :] = zs[
                        chunk, z, pl.ds(first, CORNER), :
                    ]
                rest = TILE - CORNER * len(layers)
                zc[part, d, z, pl.ds(TILE - rest, rest), :] = jnp.zeros((rest, nz), jnp.float32)

    def send_corners(part, d):
        for z in (0, 1):
            remote(
                ((1, d), (2, z)), zc.at[part, d, z], zd.at[part, d, z],
                d_ss.at[0], d_rs.at[part],
            ).start()

    def wait_corners(part):
        remote(
            ((1, 0),), zd.at[part], zd.at[part], d_ss.at[0], d_rs.at[part]
        ).wait_recv()

    def send_y(kind, d):
        _, start, size = yrows[kind]
        rows = pl.ds(start, size)
        remote(
            ((1, d),), ys.at[d, rows], yr.at[d, rows], y_ss.at[0], y_rs.at[kind]
        ).start()

    def first_rows(d):
        await_ready(1, d)
        send_corners(0, d)
        send_y(0, d)

    def bulk_down(kinds):
        for kind in kinds:
            send_y(kind, 1)
        if 4 in kinds:
            send_corners(1, 1)

    def early(m):
        v = SPEEDS[m][1]
        return (0, ny) if v == 0 else (TILE, ny - TILE) if v > 0 else (0, ny - TILE)

    def late(m):
        return (0, TILE) if SPEEDS[m][1] > 0 else (ny - TILE, TILE)

    def outgoing(x, chosen):
        return [m for m in range(Q) if crossing(m, x, nx) is not None and chosen(SPEEDS[m])]

    def send_edge(x):
        for m in outgoing(x, lambda c: c[2] == 0):
            send_x(m, 1, x, early(m))

    def send_tilted(x):
        for m in outgoing(x, lambda c: c[2] > 0):
            send_x(m, 2, x, early(m))

    def send_late(x, tilted):
        for m in outgoing(x, lambda c: c[1] != 0 and (c[2] > 0 if tilted else c[2] == 0)):
            send_x(m, 1 + tilted, x, late(m))

    def work(x, chunk, packed, between):
        slot = [{m: (s, c) for m, at, s, c in zcols[chunk][d] if at == x} for d in (0, 1)]

        def emit(m, value):
            cz = SPEEDS[m][2]
            if cz:
                d = 0 if cz > 0 else 1
                start, count = slot[d][m]
                shift = (start + count if d == 0 else start) % nz
                moved = pltpu.roll(value, shift, 1) if shift else value
                mask = (lane >= start) & (lane < start + count)
                packed[d] = jnp.where(mask, moved, packed[d])
                value = pltpu.roll(value, cz % nz, 1)
            ext[m, place(m, x), rows_at(m), :] = value

        emit_rest, emit_pairs = collide(lambda m: g[m, x], r[x])
        emit_pairs(EDGE, emit)
        between()
        emit_rest(emit)
        emit_pairs(REST, emit)

    def settle_z(chunk, chosen):
        for d in (0, 1):
            base = zr[chunk, d]
            for m, x, start, count in zcols[chunk][d]:
                if not chosen(m, x):
                    continue
                shift = (start if d == 0 else start + count) % nz
                moved = pltpu.roll(base, nz - shift, 1) if shift else base
                mask = lane < count if d == 0 else lane >= nz - count
                where = (m, place(m, x), rows_at(m), slice(None))
                ext[where] = jnp.where(mask, moved, ext[where])

    def pack_y(kind):
        tables, first, _ = yrows[kind]
        for d in (0, 1):
            for m, x, start, count in tables[d]:
                edge = PY + ny if d == 0 else PY - count
                ys[d, pl.ds(first + start, count), :] = ext[
                    m, place(m, x), pl.ds(edge, count), :
                ]

    def settle_y(kind, chosen):
        tables, first, _ = yrows[kind]
        for d in (0, 1):
            for m, x, start, count in tables[d]:
                if not chosen(m, x):
                    continue
                home = PY if d == 0 else PY + ny - count
                rows = yr[d, pl.ds(first + start, count), :]
                cz = SPEEDS[m][2]
                if cz:
                    z = 0 if cz > 0 else 1
                    rows = corner(d, z, m, x, rows)
                ext[m, place(m, x), pl.ds(home, count), :] = rows

    def corner(d, z, m, x, rows):
        chunk = next(n for n, layers in enumerate(chunks) if x in layers)
        start, width = next((s, c) for k, at, s, c in zcols[chunk][z] if (k, at) == (m, x))
        count = abs(SPEEDS[m][1])
        shift = (start if z == 0 else start + width) % nz
        tile = zd[min(chunk, 1), d, z]
        moved = pltpu.roll(tile, nz - shift, 1) if shift else tile
        first = CORNER * max(chunk - 1, 0) + (CORNER - count if d == 0 else 0)
        moved = moved[first : first + count]
        line = lane[:count]
        return jnp.where(line < width if z == 0 else line >= nz - width, moved, rows)

    def crosses(m, x):
        return crossing(m, x, nx) is not None

    def stays(m, x):
        return crossing(m, x, nx) is None

    blank = jnp.zeros((ny, nz), jnp.float32)
    for chunk, layers in enumerate(chunks):
        packed = [blank, blank]
        for n, x in enumerate(layers):
            if chunk < 2:
                loads[2 * chunk + n].wait()
            elif n == 0:
                loads[4].wait()
            if x == order[0]:
                loads[5].wait()

            def between(x=x):
                if x == order[0]:
                    await_ready(0)
                send_edge(x)
                if x == order[3]:
                    wait(ready.at[4], source[0] + source[1])
                    ferry_when(source, board)

            work(x, chunk, packed, between)
            if chunk == 2 and n == 1:
                pack_y(3)
                send_y(3, 0)
                pl.when(me[1] == 1)(lambda: bulk_down((3,)))
        for d in (0, 1):
            zs[chunk, d] = packed[d]
        if chunk == 0:
            await_ready(2)
        send_z(chunk)
        if chunk == 0:
            pack_y(1)
            pl.when(last[0] == 1)(lambda: send_y(1, 0))
        if chunk == 1:
            pack_corners(0)
            pack_y(0)
            pack_y(2)
            first_rows(0)
            pl.when(last[0] == 0)(lambda: send_y(1, 0))
            send_y(2, 0)
            pl.when(above[1][1] == 0)(lambda: first_rows(1))
            pl.when(me[1] == 1)(lambda: bulk_down((1, 2)))
    pack_y(4)
    pack_corners(1)
    send_y(4, 0)
    send_corners(1, 0)
    pl.when(me[1] == 1)(lambda: bulk_down((4,)))

    def wait_z(chunk):
        remote(((2, 0),), zs.at[chunk], zr.at[chunk], z_ss.at[0], z_rs.at[chunk]).wait_recv()

    ferry_when(carrier, carry)
    wait_z(0)
    settle_z(0, crosses)
    for x in chunks[0]:
        send_tilted(x)
    wait_z(1)
    settle_z(1, crosses)
    for x in chunks[1]:
        send_tilted(x)

    pl.when(above[1][1] == 1)(lambda: first_rows(1))
    pl.when(me[1] != 1)(lambda: bulk_down((1, 2, 3, 4)))
    settle_z(0, stays)
    settle_z(1, stays)

    def wait_y(kind):
        _, first, size = yrows[kind]
        part = (slice(None), pl.ds(first, size))
        remote(((1, 0),), ys.at[part], yr.at[part], y_ss.at[0], y_rs.at[kind]).wait_recv()

    wait_y(0)
    settle_y(0, lambda m, x: SPEEDS[m][2] == 0)
    for x in order:
        send_late(x, 0)
    wait_corners(0)
    settle_y(0, lambda m, x: SPEEDS[m][2] != 0)
    for x in order:
        send_late(x, 1)
    wait_z(2)
    settle_z(2, stays)
    wait_corners(1)
    for kind in range(1, 5):
        wait_y(kind)
        settle_y(kind, stays)
    units = sum(abs(c[0]) for c in SPEEDS)
    layers = max(n for n in range(1, nx + 1) if units % n == 0)
    span = ext.at[pl.ds(0, units // layers), pl.ds(0, layers), pl.ds(PY, ny)]
    everything = remote(((0, 0),), span, span, x_ss.at[0], x_rs.at[0])
    everything.wait_recv()
    everything.wait_send()
    ferry_when(carrier, carried)
    remote(((1, 0),), ys, ys, y_ss.at[0], y_rs.at[0]).wait_send()
    remote(((1, 0),), zc, zd, d_ss.at[0], d_rs.at[0]).wait_send()
    remote(((2, 0),), zs, zs, z_ss.at[0], z_rs.at[0]).wait_send()


def crop(ext, out, sem):
    nx, ny = out.shape[1:3]
    inside = ext.at[:, pl.ds(PX, nx), pl.ds(PY, ny)]
    for m in range(Q):
        for x in range(nx):
            pltpu.make_async_copy(inside.at[m, x], out.at[m, x], sem).start()
    pltpu.make_async_copy(inside, out, sem).wait()


def per_device(populations, relax):
    nx, ny, nz = relax.shape
    shape = (Q, nx + 2 * PX, ny + 2 * PY, nz)
    height = plan(nx)[4]
    f32 = jnp.float32
    dma = pltpu.SemaphoreType.DMA
    any_space = pl.BlockSpec(memory_space=pl.ANY)
    room = 67043328 - 4 * math.prod(shape) - 32768
    ext = pl.pallas_call(
        kernel,
        out_shape=pltpu.VMEM(shape, f32),
        in_specs=[pl.BlockSpec(memory_space=pltpu.HBM)] * 2,
        out_specs=pl.BlockSpec(memory_space=pltpu.VMEM),
        scratch_shapes=[
            pltpu.VMEM((Q, nx, ny, nz), f32),
            pltpu.VMEM((nx, ny, nz), f32),
            pltpu.VMEM((3, 2, ny, nz), f32),
            pltpu.VMEM((3, 2, ny, nz), f32),
            pltpu.VMEM((2, 2, 2, TILE, nz), f32),
            pltpu.VMEM((2, 2, 2, TILE, nz), f32),
            pltpu.VMEM((2, height, nz), f32),
            pltpu.VMEM((2, height, nz), f32),
            pltpu.VMEM((2, max(1, *FERRY), ny, nz), f32),
            dma((6,)),
            dma((1,)), dma((3,)),
            dma((1,)), dma((2,)),
            dma((1,)), dma((5,)),
            dma((1,)), dma((1,)),
            dma((2,)), dma((2,)),
            pltpu.SemaphoreType.REGULAR((5,)),
        ],
        compiler_params=pltpu.CompilerParams(
            collective_id=0, has_side_effects=True, vmem_limit_bytes=room
        ),
    )(populations, relax)
    return pl.pallas_call(
        crop,
        out_shape=jax.ShapeDtypeStruct((Q, nx, ny, nz), f32),
        in_specs=[any_space],
        out_specs=any_space,
        scratch_shapes=[dma],
        compiler_params=pltpu.CompilerParams(vmem_limit_bytes=2**20),
    )(ext)


def solution(mesh):
    return jax.shard_map(
        per_device,
        mesh=mesh,
        in_specs=(P(None, "gx", "gy", "gz"), P("gx", "gy", "gz")),
        out_specs=P(None, "gx", "gy", "gz"),
        check_vma=False,
    )
```

```python
import math

import jax
import jax.numpy as jnp
from jax import lax
from jax.experimental import pallas as pl
from jax.experimental.pallas import tpu as pltpu
from jax.sharding import PartitionSpec as P

MESH = pl.DeviceIdType.MESH
AXES = ("gx", "gy", "gz")
PX = 3
PY = 8
TILE = 8
CORNER = 2
FERRY = (2, 1)


def lattice():
    speeds = [(0, 0, 0)]
    weights = [1.0 / 12.0]
    for axis in range(3):
        for sign in (1, -1):
            vector = [0, 0, 0]
            vector[axis] = sign
            speeds.append(tuple(vector))
            weights.append(1.0 / 12.0)
    for first in (1, -1):
        for second in (1, -1):
            for third in (1, -1):
                speeds.append((first, second, third))
                weights.append(1.0 / 27.0)
    for axis in range(3):
        for sign in (2, -2):
            vector = [0, 0, 0]
            vector[axis] = sign
            speeds.append(tuple(vector))
            weights.append(2.0 / 135.0)
    for couple in ((0, 1), (0, 2), (1, 2)):
        for first in (2, -2):
            for second in (2, -2):
                vector = [0, 0, 0]
                vector[couple[0]] = first
                vector[couple[1]] = second
                speeds.append(tuple(vector))
                weights.append(1.0 / 432.0)
    for axis in range(3):
        for sign in (3, -3):
            vector = [0, 0, 0]
            vector[axis] = sign
            speeds.append(tuple(vector))
            weights.append(1.0 / 1620.0)
    return (speeds, weights)


SPEEDS, WEIGHTS = lattice()
Q = len(SPEEDS)
SQUARES = [sum(v * v for v in c) for c in SPEEDS]
PAIRS = [
    (m, SPEEDS.index(tuple(-v for v in SPEEDS[m])))
    for m in range(1, Q)
    if m < SPEEDS.index(tuple(-v for v in SPEEDS[m]))
]


EDGE = [
    (m, o) for m, o in PAIRS if SPEEDS[m][2] == 0 and SPEEDS[m][0] != 0
]
REST = [pair for pair in PAIRS if pair not in EDGE]
PURE = [(m, o) for m, o in EDGE if SPEEDS[m][1] == 0]


def crossing(m, x, nx):
    at = x + SPEEDS[m][0]
    return 0 if at >= nx else 1 if at < 0 else None


def slots(axis, sign, layers, keep):
    rows, start = [], 0
    for x in layers:
        for m, c in enumerate(SPEEDS):
            count = c[axis] * sign
            if count > 0 and keep(m, x):
                rows.append((m, x, start, count))
                start += count
    return rows, start


def plan(nx):
    order = []
    for x in range((nx + 1) // 2):
        order += [x] if x == nx - 1 - x else [x, nx - 1 - x]
    chunks = [order[:2], order[2:4], order[4:]]
    zcols = [
        [slots(2, sign, layers, lambda m, x: True)[0] for sign in (1, -1)]
        for layers in chunks
    ]
    stages = chunks[:2] + [order[4:6], order[6:]]
    yrows, start = [], 0
    kinds = [(order, True)] + [(layers, False) for layers in stages]
    for layers, out in kinds:
        both = [
            slots(1, sign, layers, lambda m, x: (crossing(m, x, nx) is not None) == out)
            for sign in (1, -1)
        ]
        size = -(-max(n for _, n in both) // TILE) * TILE
        yrows.append(([rows for rows, _ in both], start, size))
        start += size
    return order, chunks, zcols, yrows, start


def add_all(terms):
    total = terms[0]
    for term in terms[1:]:
        total = total + term
    return total


def collide(load, rate):
    sums = {k: [] for k in (1, 3, 4, 8, 9)}
    flows = {k: [[], [], []] for k in (1, 3, 4, 8, 9)}
    for m, o in PAIRS:
        up, down = load(m), load(o)
        k = SQUARES[m]
        sums[k].append(up + down)
        diff = up - down
        for axis in range(3):
            if SPEEDS[m][axis] > 0:
                flows[k][axis].append((1, diff))
            elif SPEEDS[m][axis] < 0:
                flows[k][axis].append((-1, diff))
    weight = {SQUARES[m]: WEIGHTS[m] for m in range(Q)}
    size = {1: 1, 3: 1, 4: 2, 8: 2, 9: 3}
    rest = load(0)
    groups = {k: add_all(sums[k]) for k in sums}
    rho = weight[0] * rest
    energy = None
    for k in sums:
        part = weight[k] * groups[k]
        rho = rho + part
        part = part if k == 1 else float(k) * part
        energy = part if energy is None else energy + part
    flux = []
    for axis in range(3):
        total = None
        for k in flows:
            part = None
            for sign, diff in flows[k][axis]:
                if part is None:
                    part = diff if sign > 0 else -diff
                else:
                    part = part + diff if sign > 0 else part - diff
            part = (weight[k] * size[k]) * part
            total = part if total is None else total + part
        flux.append(total)
    inverse = 1.0 / rho
    velocity = [part * inverse for part in flux]
    norm = velocity[0] * velocity[0] + velocity[1] * velocity[1] + velocity[2] * velocity[2]
    t = (energy * inverse - norm) * 0.5 - 1.0
    b = 1.5 * norm
    w = [1.5 * part for part in velocity]
    keep = 1.0 - rate
    k0 = rho * rate
    k24 = k0 * (1.0 / 24.0)
    k6 = k0 * (1.0 / 6.0)
    half_b = 0.5 * b
    kt = k0 * t
    ktb = kt * b
    ktt = kt * t
    base = k0 * (1.0 - half_b + 0.5 * half_b * half_b)
    base1 = k0 * (0.5 - 0.5 * half_b)
    baseo = k0 * (1.0 - half_b)

    def even0(s):
        return (
            base
            + kt * (0.5 * (s - 3.0))
            + ktb * (0.25 * (5.0 - s))
            + ktt * ((s * s - 10.0 * s + 15.0) / 8.0)
        )

    def emit_rest(emit):
        emit(0, keep * rest + even0(0.0))

    def emit_pairs(pairs, emit):
        for k in sums:
            chosen = [pair for pair in pairs if SQUARES[pair[0]] == k]
            if not chosen:
                continue
            s = 1.5 * k
            e0 = even0(s)
            e1 = base1 + kt * (0.25 * (s - 7.0))
            o1 = baseo + kt * (0.5 * (s - 5.0))
            for m, o in chosen:
                a = None
                for axis in range(3):
                    v = SPEEDS[m][axis]
                    if v == 0:
                        continue
                    unit = w[axis]
                    if a is None:
                        a = unit if v > 0 else -unit
                    else:
                        a = a + unit if v > 0 else a - unit
                if size[k] != 1:
                    a = float(size[k]) * a
                q = a * a
                even = e0 + q * (e1 + q * k24)
                odd = a * (o1 + q * k6)
                emit(m, keep * load(m) + (even + odd))
                emit(o, keep * load(o) + (even - odd))

    return emit_rest, emit_pairs


def kernel(
    pop, rate, ext, g, r, zs, zr, zc, zd, ys, yr, hop,
    in_sem, ss, z_rs, d_rs, y_rs, x_rs, h_ss, h_rs, ready,
):
    nx, ny, nz = pop.shape[1:]
    order, chunks, zcols, yrows, _ = plan(nx)
    head, tail = pl.ds(TILE, TILE), pl.ds(2 * TILE, ny - 2 * TILE)

    def load(first, count, rows, n):
        part = (slice(None), pl.ds(first, count), rows)
        return pltpu.make_async_copy(pop.at[part], g.at[part], in_sem.at[n])

    every = pl.ds(0, ny)
    start_order = [
        load(order[0], 1, head, 0),
        pltpu.make_async_copy(rate, r, in_sem.at[1]),
        load(order[0], 1, pl.ds(0, TILE), 2),
        load(order[0], 1, tail, 2),
        load(order[1], 1, every, 3),
    ] + [load(x, 1, every, 4) for x in order[2:4]] + [load(2, nx - 4, every, 5)]
    arrived = [
        load(order[0], 1, head, 0),
        pltpu.make_async_copy(rate, r, in_sem.at[1]),
        load(order[0], 1, pl.ds(0, ny - TILE), 2),
        load(order[1], 1, every, 3),
        load(0, 2, every, 4),
        load(2, nx - 4, every, 5),
    ]

    around, above, nears = [], [], []
    for axis in AXES:
        n = lax.axis_size(axis)
        me = lax.axis_index(axis)
        near = (lax.rem(me + 1, n), lax.rem(me + n - 1, n))
        nears.append(near)
        around.append(tuple({axis: at} for at in near))
        above.append(tuple(jnp.where(at > me, 1, 0) for at in near))
    barrier = pltpu.get_barrier_semaphore()

    links = [
        (((0, d),), 0) for d in (0, 1)
    ] + [
        (((2, d),), 1) for d in (0, 1)
    ] + [
        (((1, d), (2, z))[: 1 if z is None else 2], 2 + d)
        for d in (0, 1) for z in (None, 0, 1)
    ]

    def at(steps):
        return {name: v for axis, d in steps for name, v in around[axis][d].items()}

    size = [lax.axis_size(axis) for axis in AXES]
    me = [lax.axis_index(axis) for axis in AXES]
    last = [jnp.where(me[1] == end, 1, 0) for end in (size[1] - 1, 0)]
    chip = me[2] // 2
    apart = [
        jnp.where((n // 2 != chip) & (jnp.maximum(n, me[2]) - jnp.minimum(n, me[2]) == 1), 1, 0)
        for n in nears[2]
    ]

    def is_above(steps):
        (axis, d), z = steps[0], steps[-1][1]
        if len(steps) == 1:
            return above[axis][d]
        aside = (1 - last[d]) * apart[z]
        return (1 - aside) * above[axis][d] + aside * above[2][z]

    def signal(semaphore, steps):
        pl.semaphore_signal(semaphore, inc=1, device_id=at(steps), device_id_type=MESH)

    def wait(semaphore, amount):
        pl.when(amount > 0)(lambda: pl.semaphore_wait(semaphore, amount))

    ferry = [
        [(SPEEDS.index((PX, 0, 0)), nx - 1 - n) for n in range(FERRY[0])],
        [(SPEEDS.index((-PX, 0, 0)), n) for n in range(FERRY[1])],
    ]
    into = [jnp.where((nears[0][d] == 0) & (me[1] == 0), 1, 0) for d in (0, 1)]
    source = [jnp.where(chip == 0, into[d], 0) for d in (0, 1)]
    carrier = [jnp.where(chip == 1, into[d], 0) for d in (0, 1)]
    final = jnp.where((me[0] == 0) & (me[1] == 0) & (chip == 0), 1, 0)
    beyond = {AXES[2]: lax.rem(me[2] + 2, size[2])}
    before = {AXES[2]: lax.rem(me[2] + size[2] - 2, size[2])}

    def signal_to(semaphore, target):
        pl.semaphore_signal(semaphore, inc=1, device_id=target, device_id_type=MESH)

    for steps, _ in links:
        pl.when(is_above(steps) == 1)(lambda p=steps: signal(barrier, p))
    for d in (0, 1):
        pl.when(source[d] == 1)(lambda: signal_to(barrier, beyond))
        pl.when(final == 1)(lambda d=d: signal_to(barrier, {**around[0][1 - d], **beyond}))
    for copy in start_order:
        copy.start()
    wait(
        barrier,
        sum(1 - is_above(steps) for steps, _ in links) + 2 * (carrier[0] + carrier[1]),
    )
    for steps, flag in links:
        back = 5 - flag if flag > 1 else flag
        pl.when(is_above(steps) == 0)(lambda p=steps, f=back: signal(ready.at[f], p))
    for d in (0, 1):
        pl.when(carrier[d] == 1)(lambda: signal_to(ready.at[4], before))

    def await_ready(axis, d=None):
        flag = 2 + d if axis == 1 else axis // 2
        wait(ready.at[flag], sum(is_above(steps) for steps, f in links if f == flag))

    lane = lax.broadcasted_iota(jnp.int32, (ny, nz), 1)

    def rows_at(m):
        return pl.ds(PY + SPEEDS[m][1], ny)

    def place(m, x):
        return PX + x + SPEEDS[m][0]

    def remote(steps, src, dst, ss, rs):
        return pltpu.make_async_remote_copy(
            src_ref=src, dst_ref=dst, send_sem=ss, recv_sem=rs,
            device_id=at(steps), device_id_type=MESH,
        )

    def x_copy(m, members, x, rows):
        d = crossing(m, x, nx)
        at_x = place(m, x)
        home = at_x - nx if d == 0 else at_x + nx
        which, rows = pl.ds(m, members), pl.ds(PY + rows[0], rows[1])
        return remote(
            ((0, d),), ext.at[which, pl.ds(at_x, 1), rows], ext.at[which, pl.ds(home, 1), rows],
            ss.at[0], x_rs.at[0],
        )

    def send_x(m, members, x, rows):
        copy = x_copy(m, members, x, rows)
        d = crossing(m, x, nx)
        if (m, x) in ferry[d]:
            pl.when(source[d] == 0)(copy.start)
        else:
            copy.start()

    def board(d):
        for n, (m, x) in enumerate(ferry[d]):
            pltpu.make_async_remote_copy(
                src_ref=ext.at[m, place(m, x), pl.ds(PY, ny)], dst_ref=hop.at[d, n],
                send_sem=ss.at[0], recv_sem=h_rs.at[d],
                device_id=beyond, device_id_type=MESH,
            ).start()

    def carry(d):
        span = hop.at[d, pl.ds(0, len(ferry[d]))]
        landed = remote(((2, 0),), span, span, h_ss.at[d], h_rs.at[d])
        landed.wait_recv()
        for n, (m, x) in enumerate(ferry[d]):
            at_x = place(m, x)
            home = at_x - nx if d == 0 else at_x + nx
            pltpu.make_async_remote_copy(
                src_ref=hop.at[d, n], dst_ref=ext.at[m, home, pl.ds(PY, ny)],
                send_sem=h_ss.at[d], recv_sem=x_rs.at[0],
                device_id={**around[0][d], **before}, device_id_type=MESH,
            ).start()

    def carried(d):
        span = hop.at[d, pl.ds(0, len(ferry[d]))]
        remote(((2, 0),), span, span, h_ss.at[d], h_rs.at[d]).wait_send()

    def ferry_when(role, act):
        for d in (0, 1):
            if ferry[d]:
                pl.when(role[d] == 1)(lambda d=d: act(d))

    def send_z(chunk):
        for d in (0, 1):
            remote(
                ((2, d),), zs.at[chunk, d], zr.at[chunk, d], ss.at[0], z_rs.at[chunk]
            ).start()

    def pack_corners(part):
        layers = (0,) if part == 0 else range(1, len(chunks))
        for d in (0, 1):
            first = ny - CORNER if d == 0 else 0
            for z in (0, 1):
                for n, chunk in enumerate(layers):
                    zc[part, d, z, pl.ds(CORNER * n, CORNER), :] = zs[
                        chunk, z, pl.ds(first, CORNER), :
                    ]
                rest = TILE - CORNER * len(layers)
                zc[part, d, z, pl.ds(TILE - rest, rest), :] = jnp.zeros((rest, nz), jnp.float32)

    def send_corners(part, d):
        for z in (0, 1):
            remote(
                ((1, d), (2, z)), zc.at[part, d, z], zd.at[part, d, z],
                ss.at[0], d_rs.at[part],
            ).start()

    def wait_corners(part):
        remote(
            ((1, 0),), zd.at[part], zd.at[part], ss.at[0], d_rs.at[part]
        ).wait_recv()

    def send_y(kind, d):
        _, start, size = yrows[kind]
        rows = pl.ds(start, size)
        remote(
            ((1, d),), ys.at[d, rows], yr.at[d, rows], ss.at[0], y_rs.at[min(kind, 1)]
        ).start()

    def first_rows(d):
        await_ready(1, d)
        send_corners(0, d)
        send_y(0, d)

    def bulk_down(kinds):
        for kind in kinds:
            send_y(kind, 1)
        if 4 in kinds:
            send_corners(1, 1)

    def early(m):
        v = SPEEDS[m][1]
        return (0, ny) if v == 0 else (TILE, ny - TILE) if v > 0 else (0, ny - TILE)

    def late(m):
        return (0, TILE) if SPEEDS[m][1] > 0 else (ny - TILE, TILE)

    def outgoing(x, chosen):
        return [m for m in range(Q) if crossing(m, x, nx) is not None and chosen(SPEEDS[m])]

    def is_pure(m):
        return SPEEDS[m][1] == 0 and SPEEDS[m][2] == 0

    def send_edge(x):
        for m in outgoing(x, lambda c: c[2] == 0):
            if x == order[0] and is_pure(m):
                send_x(m, 1, x, (0, TILE))
                send_x(m, 1, x, (2 * TILE, ny - 2 * TILE))
            else:
                send_x(m, 1, x, early(m))

    def first_tile(x):
        def emit(m, value):
            if crossing(m, x, nx) is not None:
                ext[m, place(m, x), pl.ds(PY + TILE, TILE), :] = value

        _, emit_pairs = collide(lambda m: g[m, x, head, :], r[x, head, :])
        emit_pairs(PURE, emit)
        await_ready(0)
        for m in outgoing(x, lambda c: c[1] == 0 and c[2] == 0):
            send_x(m, 1, x, (TILE, TILE))

    def send_tilted(x):
        for m in outgoing(x, lambda c: c[2] > 0):
            send_x(m, 2, x, early(m))

    def send_late(x, tilted):
        for m in outgoing(x, lambda c: c[1] != 0 and (c[2] > 0 if tilted else c[2] == 0)):
            send_x(m, 1 + tilted, x, late(m))

    def work(x, chunk, packed, between):
        slot = [{m: (s, c) for m, at, s, c in zcols[chunk][d] if at == x} for d in (0, 1)]

        def emit(m, value):
            cz = SPEEDS[m][2]
            if cz:
                d = 0 if cz > 0 else 1
                start, count = slot[d][m]
                shift = (start + count if d == 0 else start) % nz
                moved = pltpu.roll(value, shift, 1) if shift else value
                mask = (lane >= start) & (lane < start + count)
                packed[d] = jnp.where(mask, moved, packed[d])
                value = pltpu.roll(value, cz % nz, 1)
            if x == order[0] and is_pure(m) and crossing(m, x, nx) is not None:
                for first, count in ((0, TILE), (2 * TILE, ny - 2 * TILE)):
                    part = pl.ds(PY + first, count)
                    ext[m, place(m, x), part, :] = value[first : first + count]
                return
            ext[m, place(m, x), rows_at(m), :] = value

        emit_rest, emit_pairs = collide(lambda m: g[m, x], r[x])
        emit_pairs(EDGE, emit)
        between()
        emit_rest(emit)
        emit_pairs(REST, emit)

    def rows_view(count):
        high, wide, deep = ext.shape[:3]
        a, b, c = next(
            (a, b, count // (a * b))
            for a in range(high, 0, -1) for b in range(1, wide + 1)
            if count % (a * b * TILE) == 0 and count // (a * b) <= deep
        )
        return ext.at[pl.ds(0, a), pl.ds(0, b), pl.ds(0, c)]

    def settle_z(chunk, chosen):
        for d in (0, 1):
            base = zr[chunk, d]
            for m, x, start, count in zcols[chunk][d]:
                if not chosen(m, x):
                    continue
                shift = (start if d == 0 else start + count) % nz
                moved = pltpu.roll(base, nz - shift, 1) if shift else base
                mask = lane < count if d == 0 else lane >= nz - count
                where = (m, place(m, x), rows_at(m), slice(None))
                ext[where] = jnp.where(mask, moved, ext[where])

    def pack_y(kind):
        tables, first, _ = yrows[kind]
        for d in (0, 1):
            for m, x, start, count in tables[d]:
                edge = PY + ny if d == 0 else PY - count
                ys[d, pl.ds(first + start, count), :] = ext[
                    m, place(m, x), pl.ds(edge, count), :
                ]

    def settle_y(kind, chosen):
        tables, first, _ = yrows[kind]
        for d in (0, 1):
            for m, x, start, count in tables[d]:
                if not chosen(m, x):
                    continue
                home = PY if d == 0 else PY + ny - count
                rows = yr[d, pl.ds(first + start, count), :]
                cz = SPEEDS[m][2]
                if cz:
                    z = 0 if cz > 0 else 1
                    rows = corner(d, z, m, x, rows)
                ext[m, place(m, x), pl.ds(home, count), :] = rows

    def corner(d, z, m, x, rows):
        chunk = next(n for n, layers in enumerate(chunks) if x in layers)
        start, width = next((s, c) for k, at, s, c in zcols[chunk][z] if (k, at) == (m, x))
        count = abs(SPEEDS[m][1])
        shift = (start if z == 0 else start + width) % nz
        tile = zd[min(chunk, 1), d, z]
        moved = pltpu.roll(tile, nz - shift, 1) if shift else tile
        first = CORNER * max(chunk - 1, 0) + (CORNER - count if d == 0 else 0)
        moved = moved[first : first + count]
        line = lane[:count]
        return jnp.where(line < width if z == 0 else line >= nz - width, moved, rows)

    def crosses(m, x):
        return crossing(m, x, nx) is not None

    def stays(m, x):
        return crossing(m, x, nx) is None

    blank = jnp.zeros((ny, nz), jnp.float32)
    for chunk, layers in enumerate(chunks):
        packed = [blank, blank]
        for n, x in enumerate(layers):
            if x == order[0]:
                arrived[0].wait()
                arrived[1].wait()
                first_tile(x)
                arrived[2].wait()
            elif x == order[1]:
                arrived[3].wait()
            elif n == 0:
                arrived[chunk + 3].wait()

            def between(x=x):
                send_edge(x)
                if x == order[3]:
                    wait(ready.at[4], source[0] + source[1])
                    ferry_when(source, board)

            work(x, chunk, packed, between)
            if chunk == 2 and n == 1:
                pack_y(3)
                send_y(3, 0)
                pl.when(me[1] == 1)(lambda: bulk_down((3,)))
        for d in (0, 1):
            zs[chunk, d] = packed[d]
        if chunk == 0:
            await_ready(2)
        send_z(chunk)
        if chunk == 0:
            pack_y(1)
            pl.when(last[0] == 1)(lambda: send_y(1, 0))
        if chunk == 1:
            pack_corners(0)
            pack_y(0)
            pack_y(2)
            first_rows(0)
            pl.when(last[0] == 0)(lambda: send_y(1, 0))
            send_y(2, 0)
            pl.when(above[1][1] == 0)(lambda: first_rows(1))
            pl.when(me[1] == 1)(lambda: bulk_down((1, 2)))
    pack_y(4)
    pack_corners(1)
    send_y(4, 0)
    send_corners(1, 0)
    pl.when(me[1] == 1)(lambda: bulk_down((4,)))

    def wait_z(chunk):
        remote(((2, 0),), zs.at[chunk], zr.at[chunk], ss.at[0], z_rs.at[chunk]).wait_recv()

    ferry_when(carrier, carry)
    wait_z(0)
    settle_z(0, crosses)
    for x in chunks[0]:
        send_tilted(x)
    wait_z(1)
    settle_z(1, crosses)
    for x in chunks[1]:
        send_tilted(x)

    pl.when(above[1][1] == 1)(lambda: first_rows(1))
    pl.when(me[1] != 1)(lambda: bulk_down((1, 2, 3, 4)))
    settle_z(0, stays)
    settle_z(1, stays)

    def wait_y(kinds):
        first = yrows[kinds[0]][1]
        part = (slice(None), pl.ds(first, sum(yrows[kind][2] for kind in kinds)))
        remote(
            ((1, 0),), ys.at[part], yr.at[part], ss.at[0], y_rs.at[min(kinds[0], 1)]
        ).wait_recv()

    wait_y((0,))
    settle_y(0, lambda m, x: SPEEDS[m][2] == 0)
    for x in order:
        send_late(x, 0)
    wait_corners(0)
    settle_y(0, lambda m, x: SPEEDS[m][2] != 0)
    for x in order:
        send_late(x, 1)
    wait_z(2)
    settle_z(2, stays)
    wait_corners(1)
    bulk = tuple(range(1, len(yrows)))
    wait_y(bulk)
    for kind in bulk:
        settle_y(kind, stays)
    units = sum(abs(c[0]) for c in SPEEDS)
    x_bytes = rows_view(units * ny)
    remote(((0, 0),), x_bytes, x_bytes, ss.at[0], x_rs.at[0]).wait_recv()
    total = units * ny + zs.shape[0] * 2 * ny + zc.shape[0] * 4 * TILE + 2 * ys.shape[1]
    all_bytes = rows_view(total)
    remote(((0, 0),), all_bytes, all_bytes, ss.at[0], x_rs.at[0]).wait_send()
    ferry_when(carrier, carried)


def crop(ext, out, sem):
    nx, ny = out.shape[1:3]
    inside = ext.at[:, pl.ds(PX, nx), pl.ds(PY, ny)]
    for m in range(Q):
        for x in range(nx):
            pltpu.make_async_copy(inside.at[m, x], out.at[m, x], sem).start()
    pltpu.make_async_copy(inside, out, sem).wait()


def per_device(populations, relax):
    nx, ny, nz = relax.shape
    shape = (Q, nx + 2 * PX, ny + 2 * PY, nz)
    height = plan(nx)[4]
    f32 = jnp.float32
    dma = pltpu.SemaphoreType.DMA
    any_space = pl.BlockSpec(memory_space=pl.ANY)
    room = 67043328 - 4 * math.prod(shape) - 32768
    ext = pl.pallas_call(
        kernel,
        out_shape=pltpu.VMEM(shape, f32),
        in_specs=[pl.BlockSpec(memory_space=pltpu.HBM)] * 2,
        out_specs=pl.BlockSpec(memory_space=pltpu.VMEM),
        scratch_shapes=[
            pltpu.VMEM((Q, nx, ny, nz), f32),
            pltpu.VMEM((nx, ny, nz), f32),
            pltpu.VMEM((3, 2, ny, nz), f32),
            pltpu.VMEM((3, 2, ny, nz), f32),
            pltpu.VMEM((2, 2, 2, TILE, nz), f32),
            pltpu.VMEM((2, 2, 2, TILE, nz), f32),
            pltpu.VMEM((2, height, nz), f32),
            pltpu.VMEM((2, height, nz), f32),
            pltpu.VMEM((2, max(1, *FERRY), ny, nz), f32),
            dma((6,)),
            dma((1,)),
            dma((3,)), dma((2,)), dma((2,)), dma((1,)),
            dma((2,)), dma((2,)),
            pltpu.SemaphoreType.REGULAR((5,)),
        ],
        compiler_params=pltpu.CompilerParams(
            collective_id=0, has_side_effects=True, vmem_limit_bytes=room
        ),
    )(populations, relax)
    return pl.pallas_call(
        crop,
        out_shape=jax.ShapeDtypeStruct((Q, nx, ny, nz), f32),
        in_specs=[any_space],
        out_specs=any_space,
        scratch_shapes=[dma],
        compiler_params=pltpu.CompilerParams(vmem_limit_bytes=2**20),
    )(ext)


def solution(mesh):
    return jax.shard_map(
        per_device,
        mesh=mesh,
        in_specs=(P(None, "gx", "gy", "gz"), P("gx", "gy", "gz")),
        out_specs=P(None, "gx", "gy", "gz"),
        check_vma=False,
    )
```

```python
import math

import jax
import jax.numpy as jnp
from jax import lax
from jax.experimental import pallas as pl
from jax.experimental.pallas import tpu as pltpu
from jax.sharding import PartitionSpec as P

MESH = pl.DeviceIdType.MESH
AXES = ("gx", "gy", "gz")
PX = 3
PY = 8
TILE = 8
CORNER = 2
FERRY = (2, 1)


def lattice():
    speeds = [(0, 0, 0)]
    weights = [1.0 / 12.0]
    for axis in range(3):
        for sign in (1, -1):
            vector = [0, 0, 0]
            vector[axis] = sign
            speeds.append(tuple(vector))
            weights.append(1.0 / 12.0)
    for first in (1, -1):
        for second in (1, -1):
            for third in (1, -1):
                speeds.append((first, second, third))
                weights.append(1.0 / 27.0)
    for axis in range(3):
        for sign in (2, -2):
            vector = [0, 0, 0]
            vector[axis] = sign
            speeds.append(tuple(vector))
            weights.append(2.0 / 135.0)
    for couple in ((0, 1), (0, 2), (1, 2)):
        for first in (2, -2):
            for second in (2, -2):
                vector = [0, 0, 0]
                vector[couple[0]] = first
                vector[couple[1]] = second
                speeds.append(tuple(vector))
                weights.append(1.0 / 432.0)
    for axis in range(3):
        for sign in (3, -3):
            vector = [0, 0, 0]
            vector[axis] = sign
            speeds.append(tuple(vector))
            weights.append(1.0 / 1620.0)
    return (speeds, weights)


SPEEDS, WEIGHTS = lattice()
Q = len(SPEEDS)
SQUARES = [sum(v * v for v in c) for c in SPEEDS]
PAIRS = [
    (m, SPEEDS.index(tuple(-v for v in SPEEDS[m])))
    for m in range(1, Q)
    if m < SPEEDS.index(tuple(-v for v in SPEEDS[m]))
]


EDGE = [
    (m, o) for m, o in PAIRS if SPEEDS[m][2] == 0 and SPEEDS[m][0] != 0
]
TILT = [
    (m, o) for m, o in PAIRS if SPEEDS[m][2] != 0 and SPEEDS[m][0] != 0
]
OTHER = [pair for pair in PAIRS if pair not in EDGE + TILT]
PURE = [(m, o) for m, o in EDGE if SPEEDS[m][1] == 0]


def crossing(m, x, nx):
    at = x + SPEEDS[m][0]
    return 0 if at >= nx else 1 if at < 0 else None


def slots(axis, sign, layers, keep):
    rows, start = [], 0
    for x in layers:
        for m, c in enumerate(SPEEDS):
            count = c[axis] * sign
            if count > 0 and keep(m, x):
                rows.append((m, x, start, count))
                start += count
    return rows, start


def plan(nx):
    order = []
    for x in range((nx + 1) // 2):
        order += [x] if x == nx - 1 - x else [x, nx - 1 - x]
    chunks = [order[:2], order[2:4], order[4:]]
    groups = [
        (chunks[0], lambda m, x: crossing(m, x, nx) is not None),
        (order[:4], lambda m, x: x not in order[:2] or crossing(m, x, nx) is None),
        (order[4:], lambda m, x: True),
    ]
    zcols = [
        [slots(2, sign, layers, keep)[0] for sign in (1, -1)] for layers, keep in groups
    ]
    stages = chunks[:2] + [order[4:6], order[6:]]
    yrows, start = [], 0
    kinds = [(order, True)] + [(layers, False) for layers in stages]
    for layers, out in kinds:
        both = [
            slots(1, sign, layers, lambda m, x: (crossing(m, x, nx) is not None) == out)
            for sign in (1, -1)
        ]
        size = -(-max(n for _, n in both) // TILE) * TILE
        yrows.append(([rows for rows, _ in both], start, size))
        start += size
    return order, chunks, zcols, yrows, start


def add_all(terms):
    total = terms[0]
    for term in terms[1:]:
        total = total + term
    return total


def collide(load, rate):
    sums = {k: [] for k in (1, 3, 4, 8, 9)}
    flows = {k: [[], [], []] for k in (1, 3, 4, 8, 9)}
    for m, o in PAIRS:
        up, down = load(m), load(o)
        k = SQUARES[m]
        sums[k].append(up + down)
        diff = up - down
        for axis in range(3):
            if SPEEDS[m][axis] > 0:
                flows[k][axis].append((1, diff))
            elif SPEEDS[m][axis] < 0:
                flows[k][axis].append((-1, diff))
    weight = {SQUARES[m]: WEIGHTS[m] for m in range(Q)}
    size = {1: 1, 3: 1, 4: 2, 8: 2, 9: 3}
    rest = load(0)
    groups = {k: add_all(sums[k]) for k in sums}
    rho = weight[0] * rest
    energy = None
    for k in sums:
        part = weight[k] * groups[k]
        rho = rho + part
        part = part if k == 1 else float(k) * part
        energy = part if energy is None else energy + part
    flux = []
    for axis in range(3):
        total = None
        for k in flows:
            part = None
            for sign, diff in flows[k][axis]:
                if part is None:
                    part = diff if sign > 0 else -diff
                else:
                    part = part + diff if sign > 0 else part - diff
            part = (weight[k] * size[k]) * part
            total = part if total is None else total + part
        flux.append(total)
    inverse = 1.0 / rho
    velocity = [part * inverse for part in flux]
    norm = velocity[0] * velocity[0] + velocity[1] * velocity[1] + velocity[2] * velocity[2]
    t = (energy * inverse - norm) * 0.5 - 1.0
    b = 1.5 * norm
    w = [1.5 * part for part in velocity]
    keep = 1.0 - rate
    k0 = rho * rate
    k24 = k0 * (1.0 / 24.0)
    k6 = k0 * (1.0 / 6.0)
    half_b = 0.5 * b
    kt = k0 * t
    ktb = kt * b
    ktt = kt * t
    base = k0 * (1.0 - half_b + 0.5 * half_b * half_b)
    base1 = k0 * (0.5 - 0.5 * half_b)
    baseo = k0 * (1.0 - half_b)

    def even0(s):
        return (
            base
            + kt * (0.5 * (s - 3.0))
            + ktb * (0.25 * (5.0 - s))
            + ktt * ((s * s - 10.0 * s + 15.0) / 8.0)
        )

    def emit_rest(emit):
        emit(0, keep * rest + even0(0.0))

    def emit_pairs(pairs, emit):
        for k in sums:
            chosen = [pair for pair in pairs if SQUARES[pair[0]] == k]
            if not chosen:
                continue
            s = 1.5 * k
            e0 = even0(s)
            e1 = base1 + kt * (0.25 * (s - 7.0))
            o1 = baseo + kt * (0.5 * (s - 5.0))
            for m, o in chosen:
                a = None
                for axis in range(3):
                    v = SPEEDS[m][axis]
                    if v == 0:
                        continue
                    unit = w[axis]
                    if a is None:
                        a = unit if v > 0 else -unit
                    else:
                        a = a + unit if v > 0 else a - unit
                if size[k] != 1:
                    a = float(size[k]) * a
                q = a * a
                even = e0 + q * (e1 + q * k24)
                odd = a * (o1 + q * k6)
                emit(m, keep * load(m) + (even + odd))
                emit(o, keep * load(o) + (even - odd))

    return emit_rest, emit_pairs


def kernel(
    pop, rate, ext, g, r, zs, zr, zc, zd, ys, yr, hop,
    in_sem, ss, z_rs, d_rs, y_rs, x_rs, h_ss, h_rs, ready,
):
    nx, ny, nz = pop.shape[1:]
    order, chunks, zcols, yrows, _ = plan(nx)
    head, tail = pl.ds(TILE, TILE), pl.ds(2 * TILE, ny - 2 * TILE)

    def load(first, count, rows, n):
        part = (slice(None), pl.ds(first, count), rows)
        return pltpu.make_async_copy(pop.at[part], g.at[part], in_sem.at[n])

    every = pl.ds(0, ny)
    start_order = [
        load(order[0], 1, head, 0),
        pltpu.make_async_copy(rate, r, in_sem.at[1]),
        load(order[0], 1, pl.ds(0, TILE), 2),
        load(order[0], 1, tail, 2),
        load(order[1], 1, every, 3),
    ] + [load(x, 1, every, 4) for x in order[2:4]] + [load(2, nx - 4, every, 5)]
    arrived = [
        load(order[0], 1, head, 0),
        pltpu.make_async_copy(rate, r, in_sem.at[1]),
        load(order[0], 1, pl.ds(0, ny - TILE), 2),
        load(order[1], 1, every, 3),
        load(0, 2, every, 4),
        load(2, nx - 4, every, 5),
    ]

    around, above, nears = [], [], []
    for axis in AXES:
        n = lax.axis_size(axis)
        me = lax.axis_index(axis)
        near = (lax.rem(me + 1, n), lax.rem(me + n - 1, n))
        nears.append(near)
        around.append(tuple({axis: at} for at in near))
        above.append(tuple(jnp.where(at > me, 1, 0) for at in near))
    barrier = pltpu.get_barrier_semaphore()

    links = [
        (((0, d),), 0) for d in (0, 1)
    ] + [
        (((2, d),), 1) for d in (0, 1)
    ] + [
        (((1, d), (2, z))[: 1 if z is None else 2], 2 + d)
        for d in (0, 1) for z in (None, 0, 1)
    ]

    def at(steps):
        return {name: v for axis, d in steps for name, v in around[axis][d].items()}

    size = [lax.axis_size(axis) for axis in AXES]
    me = [lax.axis_index(axis) for axis in AXES]
    last = [jnp.where(me[1] == end, 1, 0) for end in (size[1] - 1, 0)]
    chip = me[2] // 2
    apart = [
        jnp.where((n // 2 != chip) & (jnp.maximum(n, me[2]) - jnp.minimum(n, me[2]) == 1), 1, 0)
        for n in nears[2]
    ]

    def is_above(steps):
        (axis, d), z = steps[0], steps[-1][1]
        if len(steps) == 1:
            return above[axis][d]
        aside = (1 - last[d]) * apart[z]
        return (1 - aside) * above[axis][d] + aside * above[2][z]

    def signal(semaphore, steps):
        pl.semaphore_signal(semaphore, inc=1, device_id=at(steps), device_id_type=MESH)

    def wait(semaphore, amount):
        pl.when(amount > 0)(lambda: pl.semaphore_wait(semaphore, amount))

    ferry = [
        [(SPEEDS.index((PX, 0, 0)), nx - 1 - n) for n in range(FERRY[0])],
        [(SPEEDS.index((-PX, 0, 0)), n) for n in range(FERRY[1])],
    ]
    into = [jnp.where((nears[0][d] == 0) & (me[1] == 0), 1, 0) for d in (0, 1)]
    source = [jnp.where(chip == 0, into[d], 0) for d in (0, 1)]
    carrier = [jnp.where(chip == 1, into[d], 0) for d in (0, 1)]
    final = jnp.where((me[0] == 0) & (me[1] == 0) & (chip == 0), 1, 0)
    beyond = {AXES[2]: lax.rem(me[2] + 2, size[2])}
    before = {AXES[2]: lax.rem(me[2] + size[2] - 2, size[2])}

    def signal_to(semaphore, target):
        pl.semaphore_signal(semaphore, inc=1, device_id=target, device_id_type=MESH)

    for steps, _ in links:
        pl.when(is_above(steps) == 1)(lambda p=steps: signal(barrier, p))
    for d in (0, 1):
        pl.when(source[d] == 1)(lambda: signal_to(barrier, beyond))
        pl.when(final == 1)(lambda d=d: signal_to(barrier, {**around[0][1 - d], **beyond}))
    for copy in start_order:
        copy.start()
    wait(
        barrier,
        sum(1 - is_above(steps) for steps, _ in links) + 2 * (carrier[0] + carrier[1]),
    )
    for steps, flag in links:
        back = 5 - flag if flag > 1 else flag
        pl.when(is_above(steps) == 0)(lambda p=steps, f=back: signal(ready.at[f], p))
    for d in (0, 1):
        pl.when(carrier[d] == 1)(lambda: signal_to(ready.at[4], before))

    def await_ready(axis, d=None):
        flag = 2 + d if axis == 1 else axis // 2
        wait(ready.at[flag], sum(is_above(steps) for steps, f in links if f == flag))

    lane = lax.broadcasted_iota(jnp.int32, (ny, nz), 1)

    def rows_at(m):
        return pl.ds(PY + SPEEDS[m][1], ny)

    def place(m, x):
        return PX + x + SPEEDS[m][0]

    def remote(steps, src, dst, ss, rs):
        return pltpu.make_async_remote_copy(
            src_ref=src, dst_ref=dst, send_sem=ss, recv_sem=rs,
            device_id=at(steps), device_id_type=MESH,
        )

    def x_copy(m, members, x, rows):
        d = crossing(m, x, nx)
        at_x = place(m, x)
        home = at_x - nx if d == 0 else at_x + nx
        which, rows = pl.ds(m, members), pl.ds(PY + rows[0], rows[1])
        return remote(
            ((0, d),), ext.at[which, pl.ds(at_x, 1), rows], ext.at[which, pl.ds(home, 1), rows],
            ss.at[0], x_rs.at[0],
        )

    def send_x(m, members, x, rows):
        copy = x_copy(m, members, x, rows)
        d = crossing(m, x, nx)
        if (m, x) in ferry[d]:
            pl.when(source[d] == 0)(copy.start)
        else:
            copy.start()

    def board(d):
        for n, (m, x) in enumerate(ferry[d]):
            pltpu.make_async_remote_copy(
                src_ref=ext.at[m, place(m, x), pl.ds(PY, ny)], dst_ref=hop.at[d, n],
                send_sem=ss.at[0], recv_sem=h_rs.at[d],
                device_id=beyond, device_id_type=MESH,
            ).start()

    def carry(d):
        span = hop.at[d, pl.ds(0, len(ferry[d]))]
        landed = remote(((2, 0),), span, span, h_ss.at[d], h_rs.at[d])
        landed.wait_recv()
        for n, (m, x) in enumerate(ferry[d]):
            at_x = place(m, x)
            home = at_x - nx if d == 0 else at_x + nx
            pltpu.make_async_remote_copy(
                src_ref=hop.at[d, n], dst_ref=ext.at[m, home, pl.ds(PY, ny)],
                send_sem=h_ss.at[d], recv_sem=x_rs.at[0],
                device_id={**around[0][d], **before}, device_id_type=MESH,
            ).start()

    def carried(d):
        span = hop.at[d, pl.ds(0, len(ferry[d]))]
        remote(((2, 0),), span, span, h_ss.at[d], h_rs.at[d]).wait_send()

    def ferry_when(role, act):
        for d in (0, 1):
            if ferry[d]:
                pl.when(role[d] == 1)(lambda d=d: act(d))

    def send_z(chunk):
        for d in (0, 1):
            remote(
                ((2, d),), zs.at[chunk, d], zr.at[chunk, d], ss.at[0], z_rs.at[chunk]
            ).start()

    def pack_corners(part):
        layers = (0,) if part == 0 else range(1, len(chunks))
        for d in (0, 1):
            first = ny - CORNER if d == 0 else 0
            for z in (0, 1):
                for n, chunk in enumerate(layers):
                    zc[part, d, z, pl.ds(CORNER * n, CORNER), :] = zs[
                        chunk, z, pl.ds(first, CORNER), :
                    ]
                rest = TILE - CORNER * len(layers)
                zc[part, d, z, pl.ds(TILE - rest, rest), :] = jnp.zeros((rest, nz), jnp.float32)

    def send_corners(part, d):
        for z in (0, 1):
            remote(
                ((1, d), (2, z)), zc.at[part, d, z], zd.at[part, d, z],
                ss.at[0], d_rs.at[part],
            ).start()

    def wait_corners(part):
        remote(
            ((1, 0),), zd.at[part], zd.at[part], ss.at[0], d_rs.at[part]
        ).wait_recv()

    def send_y(kind, d):
        _, start, size = yrows[kind]
        rows = pl.ds(start, size)
        remote(
            ((1, d),), ys.at[d, rows], yr.at[d, rows], ss.at[0], y_rs.at[min(kind, 1)]
        ).start()

    def first_rows(d):
        await_ready(1, d)
        if d == 0:
            pl.when(last[0] == 0)(lambda: send_corners(0, 0))
        else:
            send_corners(0, 1)
        send_y(0, d)

    def bulk_down(kinds):
        for kind in kinds:
            send_y(kind, 1)
        if 4 in kinds:
            send_corners(1, 1)

    def early(m):
        v = SPEEDS[m][1]
        return (0, ny) if v == 0 else (TILE, ny - TILE) if v > 0 else (0, ny - TILE)

    def late(m):
        return (0, TILE) if SPEEDS[m][1] > 0 else (ny - TILE, TILE)

    def outgoing(x, chosen):
        return [m for m in range(Q) if crossing(m, x, nx) is not None and chosen(SPEEDS[m])]

    def is_pure(m):
        return SPEEDS[m][1] == 0 and SPEEDS[m][2] == 0

    def send_edge(x):
        for m in outgoing(x, lambda c: c[2] == 0):
            if x == order[0] and is_pure(m):
                send_x(m, 1, x, (0, TILE))
                send_x(m, 1, x, (2 * TILE, ny - 2 * TILE))
            else:
                send_x(m, 1, x, early(m))

    def first_tile(x):
        def emit(m, value):
            if crossing(m, x, nx) is not None:
                ext[m, place(m, x), pl.ds(PY + TILE, TILE), :] = value

        _, emit_pairs = collide(lambda m: g[m, x, head, :], r[x, head, :])
        emit_pairs(PURE, emit)
        await_ready(0)
        for m in outgoing(x, lambda c: c[1] == 0 and c[2] == 0):
            send_x(m, 1, x, (TILE, TILE))

    def send_tilted(x):
        for m in outgoing(x, lambda c: c[2] > 0):
            send_x(m, 2, x, early(m))

    def send_late(x, tilted):
        for m in outgoing(x, lambda c: c[1] != 0 and (c[2] > 0 if tilted else c[2] == 0)):
            send_x(m, 1 + tilted, x, late(m))

    def group(m, x):
        if x in chunks[0] and crossing(m, x, nx) is not None:
            return 0
        return 2 if x in chunks[2] else 1

    slot = {
        (m, x): (start, count)
        for table in zcols for rows in table for m, x, start, count in rows
    }

    def store(x):
        def emit(m, value):
            cz = SPEEDS[m][2]
            if cz:
                d = 0 if cz > 0 else 1
                start, count = slot[m, x]
                shift = (start + count if d == 0 else start) % nz
                moved = pltpu.roll(value, shift, 1) if shift else value
                mask = (lane >= start) & (lane < start + count)
                mine = packed[group(m, x)]
                mine[d] = jnp.where(mask, moved, mine[d])
                value = pltpu.roll(value, cz % nz, 1)
            if x == order[0] and is_pure(m) and crossing(m, x, nx) is not None:
                for first, count in ((0, TILE), (2 * TILE, ny - 2 * TILE)):
                    part = pl.ds(PY + first, count)
                    ext[m, place(m, x), part, :] = value[first : first + count]
                return
            ext[m, place(m, x), rows_at(m), :] = value

        return emit

    def layer(x):
        return collide(lambda m: g[m, x], r[x])

    def rows_view(count):
        high, wide, deep = ext.shape[:3]
        a, b, c = next(
            (a, b, count // (a * b))
            for a in range(high, 0, -1) for b in range(1, wide + 1)
            if count % (a * b * TILE) == 0 and count // (a * b) <= deep
        )
        return ext.at[pl.ds(0, a), pl.ds(0, b), pl.ds(0, c)]

    def settle_z(chunk, chosen):
        for d in (0, 1):
            base = zr[chunk, d]
            for m, x, start, count in zcols[chunk][d]:
                if not chosen(m, x):
                    continue
                shift = (start if d == 0 else start + count) % nz
                moved = pltpu.roll(base, nz - shift, 1) if shift else base
                mask = lane < count if d == 0 else lane >= nz - count
                where = (m, place(m, x), rows_at(m), slice(None))
                ext[where] = jnp.where(mask, moved, ext[where])

    def pack_y(kind):
        tables, first, _ = yrows[kind]
        for d in (0, 1):
            for m, x, start, count in tables[d]:
                edge = PY + ny if d == 0 else PY - count
                ys[d, pl.ds(first + start, count), :] = ext[
                    m, place(m, x), pl.ds(edge, count), :
                ]

    def settle_y(kind, chosen):
        tables, first, _ = yrows[kind]
        for d in (0, 1):
            for m, x, start, count in tables[d]:
                if not chosen(m, x):
                    continue
                home = PY if d == 0 else PY + ny - count
                rows = yr[d, pl.ds(first + start, count), :]
                cz = SPEEDS[m][2]
                if cz:
                    z = 0 if cz > 0 else 1
                    rows = corner(d, z, m, x, rows)
                ext[m, place(m, x), pl.ds(home, count), :] = rows

    def corner(d, z, m, x, rows):
        chunk = group(m, x)
        start, width = slot[m, x]
        count = abs(SPEEDS[m][1])
        shift = (start if z == 0 else start + width) % nz
        tile = zd[min(chunk, 1), d, z]
        moved = pltpu.roll(tile, nz - shift, 1) if shift else tile
        first = CORNER * max(chunk - 1, 0) + (CORNER - count if d == 0 else 0)
        moved = moved[first : first + count]
        line = lane[:count]
        return jnp.where(line < width if z == 0 else line >= nz - width, moved, rows)

    def crosses(m, x):
        return crossing(m, x, nx) is not None

    def stays(m, x):
        return crossing(m, x, nx) is None

    blank = jnp.zeros((ny, nz), jnp.float32)
    packed = [[blank, blank] for _ in chunks]

    def wait_z(chunk):
        remote(((2, 0),), zs.at[chunk], zr.at[chunk], ss.at[0], z_rs.at[chunk]).wait_recv()

    carries = carrier[0] + carrier[1]

    def tilted():
        for x in chunks[0]:
            send_tilted(x)

    def flush(chunk):
        for d in (0, 1):
            zs[chunk, d] = packed[chunk][d]
        if chunk:
            send_z(chunk)

    def first_z():
        await_ready(2)
        send_z(0)

    slow = apart[0] * above[2][0] + apart[1] * above[2][1]

    for n, x in enumerate(chunks[0]):
        if n == 0:
            arrived[0].wait()
            arrived[1].wait()
            first_tile(x)
        arrived[2 + n].wait()
        _, emit_pairs = layer(x)
        emit_pairs(EDGE, store(x))
        send_edge(x)
        emit_pairs(TILT, store(x))
    flush(0)
    pl.when(slow == 0)(first_z)
    pack_corners(0)
    pl.when(last[0] == 1)(lambda: send_corners(0, 0))
    for x in chunks[0]:
        emit_rest, emit_pairs = layer(x)
        emit_rest(store(x))
        emit_pairs(OTHER, store(x))
    pl.when(slow > 0)(first_z)
    pack_y(1)
    pl.when(last[0] == 1)(lambda: send_y(1, 0))

    def whole(x):
        emit_rest, emit_pairs = layer(x)
        emit_pairs(EDGE, store(x))
        send_edge(x)
        if x == order[3]:
            wait(ready.at[4], source[0] + source[1])
            ferry_when(source, board)
        emit_pairs(TILT, store(x))
        emit_rest(store(x))
        emit_pairs(OTHER, store(x))

    arrived[4].wait()
    for x in chunks[1]:
        whole(x)
    flush(1)
    pack_y(0)
    pack_y(2)
    first_rows(0)
    pl.when(last[0] == 0)(lambda: send_y(1, 0))
    send_y(2, 0)
    pl.when(above[1][1] == 0)(lambda: first_rows(1))
    pl.when(me[1] == 1)(lambda: bulk_down((1, 2)))
    arrived[5].wait()
    for n, x in enumerate(chunks[2]):
        if n == 3:
            wait_z(0)
            settle_z(0, crosses)
            pl.when(carries == 0)(tilted)
        whole(x)
        if n == 1:
            pack_y(3)
            send_y(3, 0)
            pl.when(me[1] == 1)(lambda: bulk_down((3,)))
    flush(2)
    pack_y(4)
    pack_corners(1)
    send_y(4, 0)
    send_corners(1, 0)
    pl.when(me[1] == 1)(lambda: bulk_down((4,)))

    ferry_when(carrier, carry)
    pl.when(carries > 0)(tilted)
    wait_z(1)
    settle_z(1, crosses)
    for x in chunks[1]:
        send_tilted(x)

    pl.when(above[1][1] == 1)(lambda: first_rows(1))
    pl.when(me[1] != 1)(lambda: bulk_down((1, 2, 3, 4)))
    settle_z(1, stays)

    def wait_y(kinds):
        first = yrows[kinds[0]][1]
        part = (slice(None), pl.ds(first, sum(yrows[kind][2] for kind in kinds)))
        remote(
            ((1, 0),), ys.at[part], yr.at[part], ss.at[0], y_rs.at[min(kinds[0], 1)]
        ).wait_recv()

    wait_y((0,))
    settle_y(0, lambda m, x: SPEEDS[m][2] == 0)
    for x in order:
        send_late(x, 0)
    wait_corners(0)
    settle_y(0, lambda m, x: SPEEDS[m][2] != 0)
    for x in order:
        send_late(x, 1)
    wait_z(2)
    settle_z(2, stays)
    wait_corners(1)
    bulk = tuple(range(1, len(yrows)))
    wait_y(bulk)
    for kind in bulk:
        settle_y(kind, stays)
    units = sum(abs(c[0]) for c in SPEEDS)
    x_bytes = rows_view(units * ny)
    remote(((0, 0),), x_bytes, x_bytes, ss.at[0], x_rs.at[0]).wait_recv()
    total = units * ny + zs.shape[0] * 2 * ny + zc.shape[0] * 4 * TILE + 2 * ys.shape[1]
    all_bytes = rows_view(total)
    remote(((0, 0),), all_bytes, all_bytes, ss.at[0], x_rs.at[0]).wait_send()
    ferry_when(carrier, carried)


def crop(ext, out, sem):
    nx, ny = out.shape[1:3]
    inside = ext.at[:, pl.ds(PX, nx), pl.ds(PY, ny)]
    for m in range(Q):
        for x in range(nx):
            pltpu.make_async_copy(inside.at[m, x], out.at[m, x], sem).start()
    pltpu.make_async_copy(inside, out, sem).wait()


def per_device(populations, relax):
    nx, ny, nz = relax.shape
    shape = (Q, nx + 2 * PX, ny + 2 * PY, nz)
    height = plan(nx)[4]
    f32 = jnp.float32
    dma = pltpu.SemaphoreType.DMA
    any_space = pl.BlockSpec(memory_space=pl.ANY)
    room = 67043328 - 4 * math.prod(shape) - 32768
    ext = pl.pallas_call(
        kernel,
        out_shape=pltpu.VMEM(shape, f32),
        in_specs=[pl.BlockSpec(memory_space=pltpu.HBM)] * 2,
        out_specs=pl.BlockSpec(memory_space=pltpu.VMEM),
        scratch_shapes=[
            pltpu.VMEM((Q, nx, ny, nz), f32),
            pltpu.VMEM((nx, ny, nz), f32),
            pltpu.VMEM((3, 2, ny, nz), f32),
            pltpu.VMEM((3, 2, ny, nz), f32),
            pltpu.VMEM((2, 2, 2, TILE, nz), f32),
            pltpu.VMEM((2, 2, 2, TILE, nz), f32),
            pltpu.VMEM((2, height, nz), f32),
            pltpu.VMEM((2, height, nz), f32),
            pltpu.VMEM((2, max(1, *FERRY), ny, nz), f32),
            dma((6,)),
            dma((1,)),
            dma((3,)), dma((2,)), dma((2,)), dma((1,)),
            dma((2,)), dma((2,)),
            pltpu.SemaphoreType.REGULAR((5,)),
        ],
        compiler_params=pltpu.CompilerParams(
            collective_id=0, has_side_effects=True, vmem_limit_bytes=room
        ),
    )(populations, relax)
    return pl.pallas_call(
        crop,
        out_shape=jax.ShapeDtypeStruct((Q, nx, ny, nz), f32),
        in_specs=[any_space],
        out_specs=any_space,
        scratch_shapes=[dma],
        compiler_params=pltpu.CompilerParams(vmem_limit_bytes=2**20),
    )(ext)


def solution(mesh):
    return jax.shard_map(
        per_device,
        mesh=mesh,
        in_specs=(P(None, "gx", "gy", "gz"), P("gx", "gy", "gz")),
        out_specs=P(None, "gx", "gy", "gz"),
        check_vma=False,
    )
```
